32 devices in a mesh: rep: 2 (over z, core), dp: 16 (over x, y).
Axes of the slice: x: 4, y: 4, z: 1, core: 2. Of those that a mesh axis runs over, the one named last changes fastest.
The devices are a block of a 4x4x8 slice.
Arguments:
- x: bfloat16 [32, 2048, 1024], P(('rep', 'dp')), parts along dimension 0
- dy: bfloat16 [32, 2048, 1024], P(('rep', 'dp')), parts along dimension 0
- w_gate: bfloat16 [2, 1024, 2816], replicated
- w_up: bfloat16 [2, 1024, 2816], replicated
- w_down: bfloat16 [2, 2816, 1024], replicated
- m_w_gate: float32 [2, 1024, 2816], replicated
- m_w_up: float32 [2, 1024, 2816], replicated
- m_w_down: float32 [2, 2816, 1024], replicated
- v_w_gate: float32 [2, 1024, 2816], replicated
- v_w_up: float32 [2, 1024, 2816], replicated
- v_w_down: float32 [2, 2816, 1024], replicated
Outputs:
- output 1: bfloat16 [4, 1024, 2816], P('rep'), parts along dimension 0
- output 2: bfloat16 [4, 1024, 2816], P('rep'), parts along dimension 0
- output 3: bfloat16 [4, 2816, 1024], P('rep'), parts along dimension 0
- output 4: float32 [4, 1024, 2816], P('rep'), parts along dimension 0
- output 5: float32 [4, 1024, 2816], P('rep'), parts along dimension 0
- output 6: float32 [4, 2816, 1024], P('rep'), parts along dimension 0
- output 7: float32 [4, 1024, 2816], P('rep'), parts along dimension 0
- output 8: float32 [4, 1024, 2816], P('rep'), parts along dimension 0
- output 9: float32 [4, 2816, 1024], P('rep'), parts along dimension 0
There are 2 independent parts. The reference program is written for one: setup_inputs(seed, part) draws one part's arguments, and reference() takes and returns one part's arrays. A program takes and returns all parts, laid end to end along the dimension named above; an argument that names none is the same for every part.
All inputs are finite; a program needn't handle non-finite values.
Results may differ from the reference program's by a relative error of at most 0.02.
Values are sent between devices in bfloat16 or wider.
A program may use at most 768 MiB of HBM per device.

```python
import jax
import jax.numpy as jnp
from jax import lax

SEQUENCES = 16
TOKENS = 2048
D = 1024
FF = 2816
LAYERS = 2
NAMES = ("w_gate", "w_up", "w_down")
SHAPES = {"w_gate": (LAYERS, D, FF), "w_up": (LAYERS, D, FF), "w_down": (LAYERS, FF, D)}


def bump(key, n, height):
    away = (jnp.arange(n, dtype=jnp.int32) - jax.random.randint(key, (), 0, n, jnp.int32)) % n
    return jnp.where(away < n // 8, height, 1.0)


def together(key, own, strength):
    shared = jax.random.normal(key, own.shape[1:], jnp.float32)
    return (own + strength * shared) * lax.rsqrt(1 + strength * strength)


def setup_inputs(seed: int = 0, part: int = 0) -> dict:
    kx, kdy, ka, kb, kz, kf, kh, kl, *keys = jax.random.split(jax.random.key(seed), 8 + 3 * len(NAMES))
    kx, kdy, ka, kb = (jax.random.fold_in(k, part) for k in (kx, kdy, ka, kb))
    kw, km, kv = (keys[i::3] for i in range(3))
    shape = (SEQUENCES, TOKENS, D)
    much_x, much_dy = jax.random.uniform(kz, (2,), jnp.float32, 0.0, 1.0)
    loud = 2.0 ** jax.random.uniform(jax.random.fold_in(kz, 1), (), jnp.float32, -1.0, 2.0)
    layers = 2.0 ** jax.random.uniform(kl, (LAYERS, 1, 1), jnp.float32, -1.0, 1.0)
    x = together(ka, jax.random.normal(kx, shape, jnp.float32), much_x) * bump(kf, D, 4.0)
    dy = together(kb, jax.random.normal(kdy, shape, jnp.float32), much_dy)
    drawn = {"x": x.astype(jnp.bfloat16), "dy": (loud * dy * (SEQUENCES * TOKENS) ** -0.5).astype(jnp.bfloat16)}
    for key, name in zip(kw, NAMES, strict=True):
        w = jax.random.normal(key, SHAPES[name], jnp.float32) * SHAPES[name][1] ** -0.5
        drawn[name] = (w * {"w_gate": 1.0, "w_up": bump(kh, FF, 4.0), "w_down": layers}[name]).astype(jnp.bfloat16)
    for key, name in zip(km, NAMES, strict=True):
        drawn[f"m_{name}"] = 0.1 * jax.random.normal(key, SHAPES[name], jnp.float32)
    for key, name in zip(kv, NAMES, strict=True):
        drawn[f"v_{name}"] = jax.random.uniform(key, SHAPES[name], jnp.float32, 0.005, 0.015)
    return drawn


def matmul(a, w):
    return jnp.dot(a, w, preferred_element_type=jnp.float32).astype(jnp.bfloat16)


def normed(h):
    wide = h.astype(jnp.float32)
    scale = lax.rsqrt(jnp.mean(wide**2, -1, keepdims=True) + 1e-6)
    return (wide * scale).astype(jnp.bfloat16)


def layer(h, w):
    a = normed(h)
    gate = jnp.dot(a, w["w_gate"], preferred_element_type=jnp.float32)
    up = jnp.dot(a, w["w_up"], preferred_element_type=jnp.float32)
    return h + matmul((jax.nn.silu(gate) * up).astype(jnp.bfloat16), w["w_down"])


def adamw(w, m, v, g):
    m = 0.9 * m + 0.1 * g
    v = 0.95 * v + 0.05 * g * g
    step = m * lax.rsqrt(v + 1e-8) + 0.1 * w
    return (w - 0.02 * step).astype(jnp.bfloat16), m, v


def stack(weights, h):
    return lax.scan(lambda h, w: (layer(h, w), None), h, weights)[0]


def reference(x, dy, w_gate, w_up, w_down, m_w_gate, m_w_up, m_w_down, v_w_gate, v_w_up, v_w_down):
    weights = dict(zip(NAMES, (w_gate, w_up, w_down), strict=True))

    def take(so_far, sequence):
        h, by_y = sequence
        _, back = jax.vjp(lambda w: stack(w, h), weights)
        return jax.tree.map(lambda total, term: total + term.astype(jnp.float32), so_far, back(by_y)[0]), None

    none_yet = {name: jnp.zeros(w.shape, jnp.float32) for name, w in weights.items()}
    by_weights, _ = lax.scan(take, none_yet, (x, dy))
    gradients = [by_weights[name].astype(jnp.bfloat16).astype(jnp.float32) for name in NAMES]
    new = [
        adamw(w.astype(jnp.float32), m, v, g)
        for w, m, v, g in zip((w_gate, w_up, w_down), (m_w_gate, m_w_up, m_w_down), (v_w_gate, v_w_up, v_w_down), gradients, strict=True)
    ]
    return tuple(one[which] for which in range(3) for one in new)
```

```python
import functools
import math

import jax
import jax.numpy as jnp
from jax import lax
from jax.experimental import pallas as pl
from jax.experimental.pallas import tpu as pltpu
from jax.sharding import PartitionSpec as P

MESH = pl.DeviceIdType.MESH
F32, BF16 = jnp.float32, jnp.bfloat16
PANELS = 4
LAT = 2
STAGES = 8
G_SLOTS = 2 * LAT + 1
OUT_SLOTS = 4 * LAT + 3
VMEM_LIMIT = 62 * 2**20


def dot(a, b):
    return jnp.dot(a, b, preferred_element_type=F32)


def dot_t(a, b):
    return lax.dot_general(a, b, (((1,), (1,)), ((), ())), preferred_element_type=F32)


def scale_of(wide):
    return lax.rsqrt(jnp.mean(wide**2, -1, keepdims=True) + 1e-6)


def normed(h):
    wide = h.astype(F32)
    return (wide * scale_of(wide)).astype(BF16)


def at_rows(start, size):
    return pl.ds(pl.multiple_of(start, size), size)


def forward_kernel(x_ref, wg_ref, wu_ref, wd_ref, h_ref, x_v, a_v, acc, wgb, wub, wdb, sem, wsem):
    tokens = x_v.shape[0]
    width = wgb.shape[2]
    blocks = wg_ref.shape[2] // width
    tile = min(512, tokens)

    def weights(b, slot):
        cols = at_rows(b * width, width)
        return (
            pltpu.make_async_copy(wg_ref.at[0, :, cols], wgb.at[slot], wsem.at[0, slot]),
            pltpu.make_async_copy(wu_ref.at[0, :, cols], wub.at[slot], wsem.at[1, slot]),
            pltpu.make_async_copy(wd_ref.at[0, cols, :], wdb.at[slot], wsem.at[2, slot]),
        )

    get = pltpu.make_async_copy(x_ref, x_v, sem)
    get.start()
    for c in weights(0, 0):
        c.start()
    get.wait()

    def norm(t, _):
        rows = at_rows(t * tile, tile)
        a_v[rows, :] = normed(x_v[rows, :])
        acc[rows, :] = jnp.zeros((tile, acc.shape[1]), F32)
        return _

    lax.fori_loop(0, tokens // tile, norm, 0)

    def block(b, carry):
        slot = b % 2

        @pl.when(b + 1 < blocks)
        def _next():
            for c in weights(b + 1, 1 - slot):
                c.start()

        for c in weights(b, slot):
            c.wait()

        def part(t, _):
            rows = at_rows(t * tile, tile)
            a = a_v[rows, :]
            gate, up = dot(a, wgb[slot]), dot(a, wub[slot])
            hidden = (jax.nn.silu(gate) * up).astype(BF16)
            acc[rows, :] += dot(hidden, wdb[slot])
            return _

        return lax.fori_loop(0, tokens // tile, part, carry)

    lax.fori_loop(0, blocks, block, 0)

    def out(t, _):
        rows = at_rows(t * tile, tile)
        a_v[rows, :] = x_v[rows, :] + acc[rows, :].astype(BF16)
        return _

    lax.fori_loop(0, tokens // tile, out, 0)
    put = pltpu.make_async_copy(a_v, h_ref, sem)
    put.start()
    put.wait()


def forward(x, wg, wu, wd):
    tokens, d = x.shape
    width = d // PANELS
    hbm = pl.BlockSpec(memory_space=pl.ANY)
    return pl.pallas_call(
        forward_kernel,
        out_shape=jax.ShapeDtypeStruct(x.shape, BF16),
        in_specs=[hbm] * 4,
        out_specs=hbm,
        scratch_shapes=[
            pltpu.VMEM((tokens, d), BF16),
            pltpu.VMEM((tokens, d), BF16),
            pltpu.VMEM((tokens, d), F32),
            pltpu.VMEM((2, d, width), BF16),
            pltpu.VMEM((2, d, width), BF16),
            pltpu.VMEM((2, width, d), BF16),
            pltpu.SemaphoreType.DMA,
            pltpu.SemaphoreType.DMA((3, 2)),
        ],
        compiler_params=pltpu.CompilerParams(vmem_limit_bytes=VMEM_LIMIT),
        cost_estimate=pl.CostEstimate(flops=6 * tokens * d * wg.shape[2], bytes_accessed=2 * (2 * x.size + 3 * d * wg.shape[2]), transcendentals=tokens * wg.shape[2]),
        name="forward",
    )(x, wg, wu, wd)


def backward_kernel(side, x_ref, h_ref, dy_ref, wg_ref, wu_ref, wd_ref, gg_ref, gu_ref, gd_ref,
                    a_v, at_v, ct_v, acc, wgb, wub, wdb, hidt, dgate, dup, own, part1, done,
                    sbuf, rbuf, sem, wsem, osem, ssem, rsem):
    tokens, d = a_v.shape
    panel = wgb.shape[2]
    blocks = wg_ref.shape[2] // panel
    quarter, unit = panel // side, panel // side // side
    tile = min(512, tokens)
    chunks = 2 * blocks * 3
    half = 3 * quarter + 3 * unit
    X1, X2, Y1, Y2 = 0, quarter, 3 * quarter, 3 * quarter + unit
    AY1, AY2, AX1, AX2 = half, half + 2 * unit, half + 3 * unit, half + 3 * unit + 2 * quarter

    rep, me = lax.axis_index("rep"), lax.axis_index("dp")
    px, py = me // side, me % side
    device = lambda x, y: (rep, (x % side) * side + y % side)
    near = (device(px + 1, py), device(px + side - 1, py), device(px, py + 1), device(px, py + side - 1))
    colours = ((0, (0, 1), (2, 3), px, py), (1, (2, 3), (0, 1), py, px))

    barrier = pltpu.get_barrier_semaphore()
    for n in near:
        pl.semaphore_signal(barrier, inc=1, device_id=n, device_id_type=MESH)
    pl.semaphore_wait(barrier, 4)

    def message(link, which, i):
        rows = pl.ds(which * half, half)
        return pltpu.make_async_remote_copy(
            src_ref=sbuf.at[link, i % LAT, rows],
            dst_ref=rbuf.at[link, i % (2 * LAT), rows],
            send_sem=ssem.at[which, link, i % LAT],
            recv_sem=rsem.at[which, link, i % (2 * LAT)],
            device_id=near[link],
            device_id_type=MESH,
        )

    def result(kind, c):
        slot = c % OUT_SLOTS
        number = c // 3
        layer, cols = 1 - number // blocks, at_rows((number % blocks) * panel, panel)
        if kind:
            ref = (gg_ref, gu_ref)[kind - 1]
            return [pltpu.make_async_copy(done.at[slot], ref.at[layer, :, cols], osem.at[slot])]
        return [
            pltpu.make_async_copy(done.at[slot, pl.ds(k * panel, panel)], gd_ref.at[layer, cols, pl.ds(k * panel, panel)], osem.at[slot])
            for k in range(PANELS)
        ]

    def wait_result(c):
        pltpu.make_async_copy(done.at[c % OUT_SLOTS], gg_ref.at[0, :, pl.ds(0, panel)], osem.at[c % OUT_SLOTS]).wait()

    def tick(i, k):
        sent, got = i % LAT, (i + LAT) % (2 * LAT)

        @pl.when((i >= LAT) & (i - LAT < chunks + 3 * LAT))
        def _():
            for link in range(4):
                message(link, 0, i + LAT).wait_send()
                message(link, 0, i + LAT).wait_recv()

        @pl.when((i >= 5 * LAT) & (i - LAT < chunks + 7 * LAT))
        def _():
            for link in range(4):
                message(link, 1, i + LAT).wait_send()
                message(link, 1, i + LAT).wait_recv()

        def stage(s):
            c = i - s * LAT
            return c, pl.when((c >= 0) & (c < chunks))

        def quarter_rows(p, k):
            return at_rows(p * panel + (k % side) * quarter, quarter)

        def unit_rows(p, k, j):
            return at_rows(p * panel + (k % side) * quarter + (j % side) * unit, unit)

        def unit_of(p, j):
            return at_rows(p * quarter + (j % side) * unit, unit)

        wide = lambda v: v.astype(F32)

        c0, when = stage(0)

        @when
        def _():
            for colour, one, two, p, q in colours:
                for j in range(2):
                    sbuf[one[j], sent, pl.ds(X1, quarter)] = own[c0 % G_SLOTS, quarter_rows(2 * colour + j, p + 2)]

        c1, when = stage(1)

        @when
        def _():
            slot = c1 % G_SLOTS
            for colour, one, two, p, q in colours:
                for j in range(2):
                    to = p + (1, side - 1)[j]
                    for w in range(2):
                        v = own[slot, quarter_rows(2 * colour + w, to)]
                        if w == j:
                            v = (wide(v) + wide(rbuf[one[j], got, pl.ds(X1, quarter)])).astype(BF16)
                        sbuf[one[j], sent, pl.ds(X2 + w * quarter, quarter)] = v

        c2, when = stage(2)

        @when
        def _():
            slot = c2 % G_SLOTS
            for colour, one, two, p, q in colours:
                for w in range(2):
                    rows = pl.ds(X2 + w * quarter, quarter)
                    part1[slot, colour, pl.ds(w * quarter, quarter)] = (
                        wide(own[slot, quarter_rows(2 * colour + w, p)]) + wide(rbuf[one[0], got, rows]) + wide(rbuf[one[1], got, rows])
                    )
                for j in range(2):
                    sbuf[two[j], sent, pl.ds(Y1, unit)] = part1[slot, colour, unit_of(j, q + 2)].astype(BF16)

        c3, when = stage(3)

        @when
        def _():
            slot = c3 % G_SLOTS
            for colour, one, two, p, q in colours:
                for j in range(2):
                    to = q + (1, side - 1)[j]
                    for w in range(2):
                        v = part1[slot, colour, unit_of(w, to)]
                        if w == j:
                            v = v + wide(rbuf[two[j], got, pl.ds(Y1, unit)])
                        sbuf[two[j], sent, pl.ds(Y2 + w * unit, unit)] = v.astype(BF16)

        c4, when = stage(4)

        @when
        def _():
            @pl.when(c4 >= OUT_SLOTS)
            def _():
                wait_result(c4)

            slot, to = c4 % G_SLOTS, c4 % OUT_SLOTS
            for colour, one, two, p, q in colours:
                for w in range(2):
                    rows = pl.ds(Y2 + w * unit, unit)
                    v = part1[slot, colour, unit_of(w, q)] + wide(rbuf[two[0], got, rows]) + wide(rbuf[two[1], got, rows])
                    v = v.astype(BF16)
                    done[to, unit_rows(2 * colour + w, p, q)] = v
                    for j in range(2):
                        sbuf[two[j], sent, pl.ds(AY1 + w * unit, unit)] = v

        c5, when = stage(5)

        @when
        def _():
            to = c5 % OUT_SLOTS
            for colour, one, two, p, q in colours:
                for j in range(2):
                    for w in range(2):
                        v = rbuf[two[j], got, pl.ds(AY1 + w * unit, unit)]
                        done[to, unit_rows(2 * colour + w, p, q + (side - 1, 1)[j])] = v
                        if w == j:
                            sbuf[two[j], sent, pl.ds(AY2, unit)] = v

        c6, when = stage(6)

        @when
        def _():
            to = c6 % OUT_SLOTS
            for colour, one, two, p, q in colours:
                for j in range(2):
                    done[to, unit_rows(2 * colour + j, p, q + 2)] = rbuf[two[j], got, pl.ds(AY2, unit)]
                for w in range(2):
                    v = done[to, quarter_rows(2 * colour + w, p)]
                    for j in range(2):
                        sbuf[one[j], sent, pl.ds(AX1 + w * quarter, quarter)] = v

        c7, when = stage(7)

        @when
        def _():
            to = c7 % OUT_SLOTS
            for colour, one, two, p, q in colours:
                for j in range(2):
                    for w in range(2):
                        v = rbuf[one[j], got, pl.ds(AX1 + w * quarter, quarter)]
                        done[to, quarter_rows(2 * colour + w, p + (side - 1, 1)[j])] = v
                        if w == j:
                            sbuf[one[j], sent, pl.ds(AX2, quarter)] = v

        c8, when = stage(8)

        @when
        def _():
            to = c8 % OUT_SLOTS
            for colour, one, two, p, q in colours:
                for j in range(2):
                    done[to, quarter_rows(2 * colour + j, p + 2)] = rbuf[one[j], got, pl.ds(AX2, quarter)]
            for c in result((k - 8 * LAT) % 3, c8):
                c.start()

        @pl.when(i < chunks + 3 * LAT)
        def _():
            for link in range(4):
                message(link, 0, i).start()

        @pl.when((i >= 4 * LAT) & (i < chunks + 7 * LAT))
        def _():
            for link in range(4):
                message(link, 1, i).start()

    def weights(number, slot):
        layer, cols = 1 - number // blocks, at_rows((number % blocks) * panel, panel)
        return (
            pltpu.make_async_copy(wg_ref.at[layer, :, cols], wgb.at[slot], wsem.at[0, slot]),
            pltpu.make_async_copy(wu_ref.at[layer, :, cols], wub.at[slot], wsem.at[1, slot]),
            pltpu.make_async_copy(wd_ref.at[layer, cols, :], wdb.at[slot], wsem.at[2, slot]),
        )

    def take_in(_t, _):
        rows = at_rows(_t * tile, tile)
        a = normed(a_v[rows, :])
        a_v[rows, :] = a
        at_v[:, rows] = a.T
        return _

    for c in weights(0, 0):
        c.start()
    gets = (pltpu.make_async_copy(h_ref, a_v, sem.at[0]), pltpu.make_async_copy(dy_ref, ct_v, sem.at[1]))
    for c in gets:
        c.start()
    for c in gets:
        c.wait()
    lax.fori_loop(0, tokens // tile, take_in, 0)

    def next_layer():
        get = pltpu.make_async_copy(h_ref, a_v, sem.at[0])
        get.start()
        get.wait()
        small = tile // 4

        def back(t, _):
            rows = at_rows(t * small, small)
            wide = a_v[rows, :].astype(F32)
            scale = scale_of(wide)
            by_a = acc[rows, :].astype(BF16).astype(F32)
            inner = jnp.mean(by_a * wide, -1, keepdims=True)
            by_h = by_a * scale - wide * (scale * scale * scale * inner)
            ct_v[rows, :] = ct_v[rows, :] + by_h.astype(BF16)
            return _

        lax.fori_loop(0, tokens // small, back, 0)
        get = pltpu.make_async_copy(x_ref, a_v, sem.at[0])
        get.start()
        get.wait()
        lax.fori_loop(0, tokens // tile, take_in, 0)

    def block(number, carry):
        slot = number % 2
        later = number < blocks

        pl.when(number == blocks)(next_layer)

        for c in weights(number, slot):
            c.wait()

        @pl.when(number + 1 < 2 * blocks)
        def _():
            for c in weights(number + 1, 1 - slot):
                c.start()

        def hidden(t, _):
            rows = at_rows(t * tile, tile)
            a = a_v[rows, :]
            gate, up = dot(a, wgb[slot]), dot(a, wub[slot])
            by_hidden = dot_t(ct_v[rows, :], wdb[slot]).astype(BF16).astype(F32)
            sigmoid = jax.nn.sigmoid(gate)
            silu = gate * sigmoid
            hidt[:, rows] = (silu * up).astype(BF16).T
            dup[rows, :] = (by_hidden * silu).astype(BF16)
            dgate[rows, :] = (by_hidden * up * (sigmoid + silu * (1.0 - sigmoid))).astype(BF16)
            return _

        lax.fori_loop(0, tokens // tile, hidden, 0)

        def into(first, by, w):
            def go(t, _):
                rows = at_rows(t * tile, tile)
                v = dot_t(by[rows, :], w[slot])
                if first:
                    v = jnp.where(number == 0, v, acc[rows, :] + v)
                else:
                    v = acc[rows, :] + v
                acc[rows, :] = v
                return _

            @pl.when(later)
            def _():
                lax.fori_loop(0, tokens // tile, go, 0)

        i = 3 * number
        for k in range(PANELS):
            own[i % G_SLOTS, pl.ds(k * panel, panel)] = dot(hidt[...], ct_v[:, pl.ds(k * panel, panel)]).astype(BF16)
        tick(i, 0)
        for k in range(PANELS):
            own[(i + 1) % G_SLOTS, pl.ds(k * panel, panel)] = dot(at_v[pl.ds(k * panel, panel), :], dgate[...]).astype(BF16)
        into(True, dgate, wgb)
        tick(i + 1, 1)
        for k in range(PANELS):
            own[(i + 2) % G_SLOTS, pl.ds(k * panel, panel)] = dot(at_v[pl.ds(k * panel, panel), :], dup[...]).astype(BF16)
        into(False, dup, wub)
        tick(i + 2, 2)
        return carry

    lax.fori_loop(0, 2 * blocks, block, 0)

    def drain(t, _):
        for k in range(3):
            tick(chunks + 3 * t + k, k)
        return _

    lax.fori_loop(0, (STAGES * LAT + 3) // 3, drain, 0)
    for c in range(chunks - OUT_SLOTS, chunks):
        wait_result(c)


def backward(side, x, h, dy, wg, wu, wd):
    tokens, d = x.shape
    panel = d // PANELS
    rows = 6 * (panel // side + panel // side // side)
    hbm = pl.BlockSpec(memory_space=pl.ANY)
    return pl.pallas_call(
        functools.partial(backward_kernel, side),
        out_shape=tuple(jax.ShapeDtypeStruct(w.shape, BF16) for w in (wg, wu, wd)),
        in_specs=[hbm] * 6,
        out_specs=(hbm,) * 3,
        scratch_shapes=[
            pltpu.VMEM((tokens, d), BF16),
            pltpu.VMEM((d, tokens), BF16),
            pltpu.VMEM((tokens, d), BF16),
            pltpu.VMEM((tokens, d), F32),
            pltpu.VMEM((2, d, panel), BF16),
            pltpu.VMEM((2, d, panel), BF16),
            pltpu.VMEM((2, panel, d), BF16),
            pltpu.VMEM((panel, tokens), BF16),
            pltpu.VMEM((tokens, panel), BF16),
            pltpu.VMEM((tokens, panel), BF16),
            pltpu.VMEM((G_SLOTS, d, panel), BF16),
            pltpu.VMEM((G_SLOTS, 2, 2 * panel // side, panel), F32),
            pltpu.VMEM((OUT_SLOTS, d, panel), BF16),
            pltpu.VMEM((4, LAT, rows, panel), BF16),
            pltpu.VMEM((4, 2 * LAT, rows, panel), BF16),
            pltpu.SemaphoreType.DMA((2,)),
            pltpu.SemaphoreType.DMA((3, 2)),
            pltpu.SemaphoreType.DMA((OUT_SLOTS,)),
            pltpu.SemaphoreType.DMA((2, 4, LAT)),
            pltpu.SemaphoreType.DMA((2, 4, 2 * LAT)),
        ],
        compiler_params=pltpu.CompilerParams(collective_id=0, has_side_effects=True, vmem_limit_bytes=VMEM_LIMIT),
        cost_estimate=pl.CostEstimate(flops=28 * tokens * d * wg.shape[2], bytes_accessed=4 * 3 * wg.size, transcendentals=2 * tokens * wg.shape[2]),
        name="backward",
    )(x, h, dy, wg, wu, wd)


def adamw(w, m, v, g):
    m = 0.9 * m + 0.1 * g
    v = 0.95 * v + 0.05 * g * g
    step = m * lax.rsqrt(v + 1e-8) + 0.1 * w
    return (w - 0.02 * step).astype(BF16), m, v


def solution(mesh):
    side = math.isqrt(mesh.shape["dp"])

    def step(x, dy, *arrays):
        weights, m, v = (arrays[i : i + 3] for i in (0, 3, 6))
        h = forward(x[0], *weights)
        gradients = backward(side, x[0], h, dy[0], *weights)
        new = [adamw(w.astype(F32), m, v, g.astype(F32)) for w, m, v, g in zip(weights, m, v, gradients, strict=True)]
        return tuple(one[which] for which in range(3) for one in new)

    return jax.shard_map(
        step,
        mesh=mesh,
        in_specs=(P(("rep", "dp"), None, None),) * 2 + (P(None, None, None),) * 9,
        out_specs=(P("rep", None, None),) * 9,
        check_vma=False,
    )
```

```python
import functools
import math

import jax
import jax.numpy as jnp
from jax import lax
from jax.experimental import pallas as pl
from jax.experimental.pallas import tpu as pltpu
from jax.sharding import PartitionSpec as P

MESH = pl.DeviceIdType.MESH
F32, BF16 = jnp.float32, jnp.bfloat16
PANELS = 4
LAT = 2
STAGES = 8
G_SLOTS = 2 * LAT + 2
OUT_SLOTS = 4 * LAT + 3
VMEM_LIMIT = 62 * 2**20


def dot(a, b):
    return jnp.dot(a, b, preferred_element_type=F32)


def dot_t(a, b):
    return lax.dot_general(a, b, (((1,), (1,)), ((), ())), preferred_element_type=F32)


def scale_of(wide):
    return lax.rsqrt(jnp.mean(wide**2, -1, keepdims=True) + 1e-6)


def normed(h):
    wide = h.astype(F32)
    return (wide * scale_of(wide)).astype(BF16)


def at_rows(start, size):
    return pl.ds(pl.multiple_of(start, size), size)


def forward_kernel(x_ref, wg_ref, wu_ref, wd_ref, h_ref, gu_ref, x_v, a_v, acc, wgu, wdb, gu_v, sem, wsem, gsem):
    tokens = x_v.shape[0]
    panel = wdb.shape[1]
    blocks = wg_ref.shape[2] // panel
    tile = min(512, tokens // 2)

    def weights(b, slot):
        cols = at_rows(b * panel, panel)
        return (
            pltpu.make_async_copy(wg_ref.at[0, :, cols], wgu.at[slot, :, pl.ds(0, panel)], wsem.at[0, slot]),
            pltpu.make_async_copy(wu_ref.at[0, :, cols], wgu.at[slot, :, pl.ds(panel, panel)], wsem.at[1, slot]),
            pltpu.make_async_copy(wd_ref.at[0, cols, :], wdb.at[slot], wsem.at[2, slot]),
        )

    def keep(b, slot):
        return pltpu.make_async_copy(gu_v.at[slot], gu_ref.at[b], gsem.at[slot])

    get = pltpu.make_async_copy(x_ref, x_v, sem)
    get.start()
    for c in weights(0, 0):
        c.start()
    get.wait()

    def norm(t, _):
        rows = at_rows(t * tile, tile)
        a_v[rows, :] = normed(x_v[rows, :])
        acc[rows, :] = jnp.zeros((tile, acc.shape[1]), F32)
        return _

    lax.fori_loop(0, tokens // tile, norm, 0)

    def block(b, carry):
        slot = b % 2

        @pl.when(b + 1 < blocks)
        def _():
            for c in weights(b + 1, 1 - slot):
                c.start()

        for c in weights(b, slot):
            c.wait()

        @pl.when(b >= 2)
        def _():
            keep(b, slot).wait()

        for t in range(tokens // tile):
            rows = pl.ds(t * tile, tile)
            gu = dot(a_v[rows, :], wgu[slot])
            gu_v[slot, rows, :] = gu
            hidden = (jax.nn.silu(gu[:, :panel]) * gu[:, panel:]).astype(BF16)
            acc[rows, :] += dot(hidden, wdb[slot])
        keep(b, slot).start()
        return carry

    lax.fori_loop(0, blocks, block, 0)

    def out(t, _):
        rows = at_rows(t * tile, tile)
        a_v[rows, :] = x_v[rows, :] + acc[rows, :].astype(BF16)
        return _

    lax.fori_loop(0, tokens // tile, out, 0)
    put = pltpu.make_async_copy(a_v, h_ref, sem)
    put.start()
    put.wait()
    for b in range(max(0, blocks - 2), blocks):
        keep(b, b % 2).wait()


def forward(x, wg, wu, wd):
    tokens, d = x.shape
    panel = d // PANELS
    blocks = wg.shape[2] // panel
    hbm = pl.BlockSpec(memory_space=pl.ANY)
    return pl.pallas_call(
        forward_kernel,
        out_shape=(jax.ShapeDtypeStruct(x.shape, BF16), jax.ShapeDtypeStruct((blocks, tokens, 2 * panel), F32)),
        in_specs=[hbm] * 4,
        out_specs=(hbm, hbm),
        scratch_shapes=[
            pltpu.VMEM((tokens, d), BF16),
            pltpu.VMEM((tokens, d), BF16),
            pltpu.VMEM((tokens, d), F32),
            pltpu.VMEM((2, d, 2 * panel), BF16),
            pltpu.VMEM((2, panel, d), BF16),
            pltpu.VMEM((2, tokens, 2 * panel), F32),
            pltpu.SemaphoreType.DMA,
            pltpu.SemaphoreType.DMA((3, 2)),
            pltpu.SemaphoreType.DMA((2,)),
        ],
        compiler_params=pltpu.CompilerParams(vmem_limit_bytes=VMEM_LIMIT),
        cost_estimate=pl.CostEstimate(flops=6 * tokens * d * wg.shape[2], bytes_accessed=2 * (2 * x.size + 3 * d * wg.shape[2]), transcendentals=tokens * wg.shape[2]),
        name="forward",
    )(x, wg, wu, wd)


def backward_kernel(side, x_ref, h_ref, kept_ref, dy_ref, wg_ref, wu_ref, wd_ref, g_ref, q0_ref, q1_ref, q2_ref, q3_ref,
                    a_v, at_v, ct_v, acc, wgu, wdb, hidt, dgu, own, part1, done,
                    sbuf, rbuf, sem, wsem, osem, ssem, rsem):
    tokens, d = a_v.shape
    panel = wdb.shape[1]
    blocks = wg_ref.shape[2] // panel
    quarter, unit = panel // side, panel // side // side
    tile = min(512, tokens // 4)
    first, chunks = blocks * 3, 2 * blocks * 3
    half = 3 * quarter + 3 * unit
    X1, X2, Y1, Y2 = 0, quarter, 3 * quarter, 3 * quarter + unit
    AY1, AY2, AX1, AX2 = half, half + 2 * unit, half + 3 * unit, half + 3 * unit + 2 * quarter

    rep, me = lax.axis_index("rep"), lax.axis_index("dp")
    px, py = me // side, me % side
    device = lambda x, y: (rep, (x % side) * side + y % side)
    near = (device(px + 1, py), device(px + side - 1, py), device(px, py + 1), device(px, py + side - 1))
    colours = ((0, (0, 1), (2, 3), px, py), (1, (2, 3), (0, 1), py, px))

    barrier = pltpu.get_barrier_semaphore()
    for n in near:
        pl.semaphore_signal(barrier, inc=1, device_id=n, device_id_type=MESH)
    pl.semaphore_wait(barrier, 4)

    parts = ((X1, Y1), (Y1, AX1), (AX1, 2 * half))
    sent_in = ((0, chunks + LAT), (2 * LAT, chunks + 5 * LAT), (6 * LAT, first + 7 * LAT))

    def message(link, which, i):
        rows = pl.ds(parts[which][0], parts[which][1] - parts[which][0])
        return pltpu.make_async_remote_copy(
            src_ref=sbuf.at[link, i % LAT, rows],
            dst_ref=rbuf.at[link, i % (2 * LAT), rows],
            send_sem=ssem.at[which, link, i % LAT],
            recv_sem=rsem.at[which, link, i % (2 * LAT)],
            device_id=near[link],
            device_id_type=MESH,
        )

    def take_whole(k, c):
        pltpu.make_async_copy(done.at[c % OUT_SLOTS], g_ref.at[k, (c // 3) % blocks], osem.at[c % OUT_SLOTS]).start()

    def take_quarters(k, c):
        slot = c % OUT_SLOTS
        for colour, _, _, p, _ in colours:
            for j in range(2):
                rows = at_rows((2 * colour + j) * panel + p * quarter, quarter)
                ref = (q0_ref, q1_ref, q2_ref, q3_ref)[2 * colour + j]
                pltpu.make_async_copy(done.at[slot, rows], ref.at[k, (c // 3) % blocks], osem.at[slot]).start()

    def wait_whole(c):
        pltpu.make_async_copy(done.at[c % OUT_SLOTS], g_ref.at[0, 0], osem.at[c % OUT_SLOTS]).wait()

    def wait_quarters(c):
        rows = pl.ds(0, quarter)
        for _ in range(PANELS):
            pltpu.make_async_copy(done.at[c % OUT_SLOTS, rows], q0_ref.at[0, 0], osem.at[c % OUT_SLOTS]).wait()

    def tick(i, k):
        sent, got = i % LAT, (i + LAT) % (2 * LAT)

        for which in range(3):
            start, stop = sent_in[which]

            @pl.when((i >= start + LAT) & (i < stop + LAT))
            def _(which=which):
                for link in range(4):
                    message(link, which, i + LAT).wait_send()
                    message(link, which, i + LAT).wait_recv()

        def stage(s, stop=chunks):
            c = i - s * LAT
            return c, pl.when((c >= 0) & (c < stop))

        def quarter_rows(p, k):
            return at_rows(p * panel + (k % side) * quarter, quarter)

        def unit_rows(p, k, j):
            return at_rows(p * panel + (k % side) * quarter + (j % side) * unit, unit)

        def unit_of(p, j):
            return at_rows(p * quarter + (j % side) * unit, unit)

        wide = lambda v: v.astype(F32)

        c0, when = stage(0)

        @when
        def _():
            for colour, one, two, p, q in colours:
                for j in range(2):
                    sbuf[one[j], sent, pl.ds(X1, quarter)] = own[c0 % G_SLOTS, quarter_rows(2 * colour + j, p + 2)]

        c1, when = stage(1)

        @when
        def _():
            slot = c1 % G_SLOTS
            for colour, one, two, p, q in colours:
                for j in range(2):
                    to = p + (1, side - 1)[j]
                    for w in range(2):
                        v = own[slot, quarter_rows(2 * colour + w, to)]
                        if w == j:
                            v = (wide(v) + wide(rbuf[one[j], got, pl.ds(X1, quarter)])).astype(BF16)
                        sbuf[one[j], sent, pl.ds(X2 + w * quarter, quarter)] = v

        c2, when = stage(2)

        @when
        def _():
            slot = c2 % G_SLOTS
            for colour, one, two, p, q in colours:
                for w in range(2):
                    rows = pl.ds(X2 + w * quarter, quarter)
                    part1[slot, colour, pl.ds(w * quarter, quarter)] = (
                        wide(own[slot, quarter_rows(2 * colour + w, p)]) + wide(rbuf[one[0], got, rows]) + wide(rbuf[one[1], got, rows])
                    )
                for j in range(2):
                    sbuf[two[j], sent, pl.ds(Y1, unit)] = part1[slot, colour, unit_of(j, q + 2)].astype(BF16)

        c3, when = stage(3)

        @when
        def _():
            slot = c3 % G_SLOTS
            for colour, one, two, p, q in colours:
                for j in range(2):
                    to = q + (1, side - 1)[j]
                    for w in range(2):
                        v = part1[slot, colour, unit_of(w, to)]
                        if w == j:
                            v = v + wide(rbuf[two[j], got, pl.ds(Y1, unit)])
                        sbuf[two[j], sent, pl.ds(Y2 + w * unit, unit)] = v.astype(BF16)

        c4, when = stage(4)

        @when
        def _():
            @pl.when((c4 >= OUT_SLOTS) & (c4 < first + OUT_SLOTS))
            def _():
                wait_whole(c4)

            @pl.when(c4 >= first + OUT_SLOTS)
            def _():
                wait_quarters(c4)

            slot, to = c4 % G_SLOTS, c4 % OUT_SLOTS
            for colour, one, two, p, q in colours:
                for w in range(2):
                    rows = pl.ds(Y2 + w * unit, unit)
                    v = part1[slot, colour, unit_of(w, q)] + wide(rbuf[two[0], got, rows]) + wide(rbuf[two[1], got, rows])
                    v = v.astype(BF16)
                    done[to, unit_rows(2 * colour + w, p, q)] = v
                    for j in range(2):
                        sbuf[two[j], sent, pl.ds(AY1 + w * unit, unit)] = v

        c5, when = stage(5)

        @when
        def _():
            to = c5 % OUT_SLOTS
            for colour, one, two, p, q in colours:
                for j in range(2):
                    for w in range(2):
                        v = rbuf[two[j], got, pl.ds(AY1 + w * unit, unit)]
                        done[to, unit_rows(2 * colour + w, p, q + (side - 1, 1)[j])] = v
                        if w == j:
                            sbuf[two[j], sent, pl.ds(AY2, unit)] = v

        c6, when = stage(6)

        @when
        def _():
            to = c6 % OUT_SLOTS
            for colour, one, two, p, q in colours:
                for j in range(2):
                    done[to, unit_rows(2 * colour + j, p, q + 2)] = rbuf[two[j], got, pl.ds(AY2, unit)]

            @pl.when(c6 < first)
            def _():
                for colour, one, two, p, q in colours:
                    for w in range(2):
                        v = done[to, quarter_rows(2 * colour + w, p)]
                        for j in range(2):
                            sbuf[one[j], sent, pl.ds(AX1 + w * quarter, quarter)] = v

            @pl.when(c6 >= first)
            def _():
                take_quarters((k - 6 * LAT) % 3, c6)

        c7, when = stage(7, first)

        @when
        def _():
            to = c7 % OUT_SLOTS
            for colour, one, two, p, q in colours:
                for j in range(2):
                    for w in range(2):
                        v = rbuf[one[j], got, pl.ds(AX1 + w * quarter, quarter)]
                        done[to, quarter_rows(2 * colour + w, p + (side - 1, 1)[j])] = v
                        if w == j:
                            sbuf[one[j], sent, pl.ds(AX2, quarter)] = v

        c8, when = stage(8, first)

        @when
        def _():
            to = c8 % OUT_SLOTS
            for colour, one, two, p, q in colours:
                for j in range(2):
                    done[to, quarter_rows(2 * colour + j, p + 2)] = rbuf[one[j], got, pl.ds(AX2, quarter)]
            take_whole((k - 8 * LAT) % 3, c8)

        for which in range(3):
            start, stop = sent_in[which]

            @pl.when((i >= start) & (i < stop))
            def _(which=which):
                for link in range(4):
                    message(link, which, i).start()

    def weights(number, slot):
        layer, cols = 1 - number // blocks, at_rows((number % blocks) * panel, panel)
        return (
            pltpu.make_async_copy(wg_ref.at[layer, :, cols], wgu.at[slot, :, pl.ds(0, panel)], wsem.at[0, slot]),
            pltpu.make_async_copy(wu_ref.at[layer, :, cols], wgu.at[slot, :, pl.ds(panel, panel)], wsem.at[1, slot]),
            pltpu.make_async_copy(wd_ref.at[layer, cols, :], wdb.at[slot], wsem.at[2, slot]),
        )

    def take_in(_t, _):
        rows = at_rows(_t * tile, tile)
        a = normed(a_v[rows, :])
        a_v[rows, :] = a
        at_v[:, rows] = a.T
        return _

    def columns_of(number):
        return at_rows((number % 2) * 2 * panel, 2 * panel)

    def fetch(number):
        return pltpu.make_async_copy(kept_ref.at[number - blocks], acc.at[:, columns_of(number)], sem.at[number % 2])

    for c in weights(0, 0):
        c.start()
    gets = (pltpu.make_async_copy(h_ref, a_v, sem.at[0]), pltpu.make_async_copy(dy_ref, ct_v, sem.at[1]))
    for c in gets:
        c.start()
    for c in gets:
        c.wait()
    lax.fori_loop(0, tokens // tile, take_in, 0)

    def next_layer():
        get = pltpu.make_async_copy(h_ref, a_v, sem.at[0])
        get.start()
        get.wait()
        small = tile // 4

        def back(t, _):
            rows = at_rows(t * small, small)
            wide = a_v[rows, :].astype(F32)
            scale = scale_of(wide)
            by_a = acc[rows, :].astype(BF16).astype(F32)
            inner = jnp.mean(by_a * wide, -1, keepdims=True)
            by_h = by_a * scale - wide * (scale * scale * scale * inner)
            ct_v[rows, :] = ct_v[rows, :] + by_h.astype(BF16)
            return _

        lax.fori_loop(0, tokens // small, back, 0)
        get = pltpu.make_async_copy(x_ref, a_v, sem.at[0])
        get.start()
        get.wait()
        fetch(blocks).start()
        lax.fori_loop(0, tokens // tile, take_in, 0)

    def block(number, carry):
        slot = number % 2
        later = number < blocks
        i = 3 * number

        pl.when(number == blocks)(next_layer)

        for c in weights(number, slot):
            c.wait()

        @pl.when(number + 1 < 2 * blocks)
        def _():
            for c in weights(number + 1, 1 - slot):
                c.start()

        @pl.when(number >= blocks)
        def _():
            pltpu.make_async_copy(kept_ref.at[0], acc.at[:, columns_of(number)], sem.at[slot]).wait()

            @pl.when(number + 1 < 2 * blocks)
            def _():
                fetch(number + 1).start()

        def hidden(t, gu):
            rows = pl.ds(t * tile, tile)
            by_hidden = dot_t(ct_v[rows, :], wdb[slot]).astype(BF16).astype(F32)
            gate, up = gu[:, :panel], gu[:, panel:]
            sigmoid = jax.nn.sigmoid(gate)
            silu = gate * sigmoid
            hidt[:, rows] = (silu * up).astype(BF16).T
            dgu[rows, pl.ds(0, panel)] = (by_hidden * up * (sigmoid + silu * (1.0 - sigmoid))).astype(BF16)
            dgu[rows, pl.ds(panel, panel)] = (by_hidden * silu).astype(BF16)

        def hidden_half(part):
            tiles = tokens // tile // 2

            @pl.when(later)
            def _():
                for t in range(part * tiles, part * tiles + tiles):
                    hidden(t, dot(a_v[pl.ds(t * tile, tile), :], wgu[slot]))

            @pl.when(number >= blocks)
            def _():
                for t in range(part * tiles, part * tiles + tiles):
                    hidden(t, acc[pl.ds(t * tile, tile), columns_of(number)])

        hidden_half(0)

        @pl.when(number > 0)
        def _():
            tick(i - 1, 2)

        hidden_half(1)
        for k in range(PANELS):
            own[i % G_SLOTS, pl.ds(k * panel, panel)] = dot(hidt[...], ct_v[:, pl.ds(k * panel, panel)]).astype(BF16)
        tick(i, 0)
        for k in range(PANELS):
            v = dot(at_v[pl.ds(k * panel, panel), :], dgu[...]).astype(BF16)
            own[(i + 1) % G_SLOTS, pl.ds(k * panel, panel)] = v[:, :panel]
            own[(i + 2) % G_SLOTS, pl.ds(k * panel, panel)] = v[:, panel:]
        tick(i + 1, 1)

        @pl.when(later)
        def _():
            for t in range(tokens // tile):
                rows = pl.ds(t * tile, tile)
                v = dot_t(dgu[rows, :], wgu[slot])
                acc[rows, :] = jnp.where(number == 0, v, acc[rows, :] + v)

        return carry

    lax.fori_loop(0, 2 * blocks, block, 0)

    tick(chunks - 1, 2)

    def drain(t, _):
        for k in range(3):
            tick(chunks + 3 * t + k, k)
        return _

    lax.fori_loop(0, (6 * LAT + 2) // 3, drain, 0)
    for c in range(chunks - OUT_SLOTS, chunks):
        (wait_whole if c < first else wait_quarters)(c)


def backward(side, x, h, kept, dy, wg, wu, wd):
    tokens, d = x.shape
    panel = d // PANELS
    blocks = wg.shape[2] // panel
    rows = 6 * (panel // side + panel // side // side)
    hbm = pl.BlockSpec(memory_space=pl.ANY)
    return pl.pallas_call(
        functools.partial(backward_kernel, side),
        out_shape=(jax.ShapeDtypeStruct((3, blocks, d, panel), BF16),) + (jax.ShapeDtypeStruct((3, blocks, panel // side, panel), BF16),) * 4,
        in_specs=[hbm] * 7,
        out_specs=(hbm,) * 5,
        scratch_shapes=[
            pltpu.VMEM((tokens, d), BF16),
            pltpu.VMEM((d, tokens), BF16),
            pltpu.VMEM((tokens, d), BF16),
            pltpu.VMEM((tokens, d), F32),
            pltpu.VMEM((2, d, 2 * panel), BF16),
            pltpu.VMEM((2, panel, d), BF16),
            pltpu.VMEM((panel, tokens), BF16),
            pltpu.VMEM((tokens, 2 * panel), BF16),
            pltpu.VMEM((G_SLOTS, d, panel), BF16),
            pltpu.VMEM((G_SLOTS, 2, 2 * panel // side, panel), F32),
            pltpu.VMEM((OUT_SLOTS, d, panel), BF16),
            pltpu.VMEM((4, LAT, rows, panel), BF16),
            pltpu.VMEM((4, 2 * LAT, rows, panel), BF16),
            pltpu.SemaphoreType.DMA((2,)),
            pltpu.SemaphoreType.DMA((3, 2)),
            pltpu.SemaphoreType.DMA((OUT_SLOTS,)),
            pltpu.SemaphoreType.DMA((3, 4, LAT)),
            pltpu.SemaphoreType.DMA((3, 4, 2 * LAT)),
        ],
        compiler_params=pltpu.CompilerParams(collective_id=0, has_side_effects=True, vmem_limit_bytes=VMEM_LIMIT),
        cost_estimate=pl.CostEstimate(flops=24 * tokens * d * wg.shape[2], bytes_accessed=4 * 3 * wg.size, transcendentals=2 * tokens * wg.shape[2]),
        name="backward",
    )(x, h, kept, dy, wg, wu, wd)


def adamw(w, m, v, g):
    m = 0.9 * m + 0.1 * g
    v = 0.95 * v + 0.05 * g * g
    step = m * lax.rsqrt(v + 1e-8) + 0.1 * w
    return (w - 0.02 * step).astype(BF16), m, v


RING = 4


def update_kernel(layer, side, plan, sources, fresh, *refs):
    wmv, refs = (refs[0:3], refs[3:6], refs[6:9]), refs[9:]
    source, refs = refs[:sources], refs[sources:]
    refs = refs if fresh else refs[9:]
    new, refs = (refs[0:3], refs[3:6], refs[6:9]), refs[9:]
    tall, flat, gbuf, isem, osem = refs[0:3], refs[3:6], refs[6], refs[7], refs[8]
    blocks, quarter, panel = gbuf.shape[2:]
    me = lax.axis_index("dp")
    position = (me // side, me % side)

    units = [(kind, *one) for kind in range(3) for one in plan]

    def where(u):
        kind, colour, relative, k, halves = units[u]
        k = (position[colour] + k + side) % side if relative else k
        if kind == 0:
            return (layer, slice(None), k, slice(None), pl.ds(2 * colour * panel, 2 * panel))
        return (layer, pl.ds(2 * colour, 2), k)

    def buffers(u):
        return flat if units[u][0] == 0 else tall

    def copies_in(u):
        slot, kind = u % RING, units[u][0]
        order = (2, 0, 1)[kind]
        cs = [pltpu.make_async_copy(r[order].at[where(u)], b.at[slot], isem.at[n, slot]) for n, (r, b) in enumerate(zip(wmv, buffers(u)))]
        for j, (which, rows) in enumerate(units[u][4]):
            ref = source[which]
            ref = ref.at[kind] if rows is None else ref.at[kind, :, pl.ds(rows, quarter)]
            cs.append(pltpu.make_async_copy(ref, gbuf.at[slot, j], isem.at[3 + j, slot]))
        return cs

    def copies_out(u):
        slot, order = u % RING, (2, 0, 1)[units[u][0]]
        return [pltpu.make_async_copy(b.at[slot], r[order].at[where(u)], osem.at[n, slot]) for n, (r, b) in enumerate(zip(new, buffers(u)))]

    def start(u):
        for c in copies_in(u):
            c.start()

    ahead = RING - 2
    for u in range(min(ahead, len(units))):
        start(u)
    for u in range(len(units)):
        if u + ahead < len(units):
            if u + ahead >= RING:
                for c in copies_out(u + ahead - RING):
                    c.wait()
            start(u + ahead)
        for c in copies_in(u):
            c.wait()
        slot = u % RING
        w_b, m_b, v_b = buffers(u)

        def part(b, carry):
            for j in range(2):
                if units[u][0] == 0:
                    at = (slot, b, slice(None), pl.ds(j * panel, panel))
                else:
                    at = (slot, j, slice(None), at_rows(b * panel, panel))
                w_b[at], m_b[at], v_b[at] = adamw(w_b[at].astype(F32), m_b[at], v_b[at], gbuf[slot, j, b].astype(F32))
            return carry

        lax.fori_loop(0, blocks, part, 0)
        for c in copies_out(u):
            c.start()
    for u in range(max(0, len(units) - RING), len(units)):
        for c in copies_out(u):
            c.wait()


def update(layer, side, plan, wmv, sources, old):
    gate = wmv[0]
    _, _, _, quarter, ff = gate.shape
    blocks = wmv[2].shape[1]
    panel = ff // blocks
    hbm = pl.BlockSpec(memory_space=pl.ANY)
    size = len(plan) * 3 * 2 * quarter * ff
    return pl.pallas_call(
        functools.partial(update_kernel, layer, side, plan, len(sources), old is None),
        out_shape=tuple(jax.ShapeDtypeStruct(a.shape, a.dtype) for a in wmv),
        in_specs=[hbm] * (9 + len(sources) + (0 if old is None else 9)),
        out_specs=(hbm,) * 9,
        input_output_aliases={} if old is None else {9 + len(sources) + n: n for n in range(9)},
        scratch_shapes=[pltpu.VMEM((RING, 2, quarter, ff), t) for t in (BF16, F32, F32)]
        + [pltpu.VMEM((RING, blocks, quarter, 2 * panel), t) for t in (BF16, F32, F32)]
        + [pltpu.VMEM((RING, 2, blocks, quarter, panel), BF16), pltpu.SemaphoreType.DMA((5, RING)), pltpu.SemaphoreType.DMA((3, RING))],
        compiler_params=pltpu.CompilerParams(vmem_limit_bytes=VMEM_LIMIT),
        cost_estimate=pl.CostEstimate(flops=size * 6000, bytes_accessed=22 * size, transcendentals=size),
        name=f"update_{layer}_{len(plan)}",
    )(*wmv, *sources, *(old or ()))


def solution(mesh):
    side = math.isqrt(mesh.shape["dp"])
    spots = [(x, y) for x in range(side) for y in range(side)]

    def shift(dx, dy):
        return [(x * side + y, (x + dx) % side * side + (y + dy) % side) for x, y in spots]

    ways = ((shift(1, 0), shift(-1, 0)), (shift(0, 1), shift(0, -1)))

    def step(x, dy, *arrays):
        weights = arrays[:3]
        x, dy = x[0], dy[0]
        d, ff = weights[0].shape[1:]
        panel = d // PANELS
        quarter, blocks = panel // side, ff // panel
        h, kept = forward(x, *weights)
        whole, *quarters = backward(side, x, h, kept, dy, *weights)
        wmv = [a.reshape(a.shape[0], blocks, side, quarter, d) if n % 3 == 2 else a.reshape(a.shape[0], PANELS, side, quarter, ff) for n, a in enumerate(arrays)]

        left = [lax.ppermute(q, "dp", ways[n // 2][0]) for n, q in enumerate(quarters)]
        right = [lax.ppermute(q, "dp", ways[n // 2][1]) for n, q in enumerate(quarters)]
        plan = [(c, False, k, [(0, (2 * c + j) * panel + k * quarter) for j in range(2)]) for c in range(2) for k in range(side)]
        new = update(1, side, plan, wmv, [whole], None)
        far = [lax.ppermute((left, right)[n % 2][n], "dp", ways[n // 2][n % 2]) for n in range(4)]
        plan = [(c, True, r, [(4 * s + 2 * c + j, None) for j in range(2)]) for c in range(2) for s, r in enumerate((0, -1, 1))]
        new = update(0, side, plan, wmv, [*quarters, *left, *right], new)
        plan = [(c, True, 2, [(2 * c + j, None) for j in range(2)]) for c in range(2)]
        new = update(0, side, plan, wmv, far, new)
        return tuple(a.reshape(b.shape) for a, b in zip(new, arrays, strict=True))

    return jax.shard_map(
        step,
        mesh=mesh,
        in_specs=(P(("rep", "dp"), None, None),) * 2 + (P(None, None, None),) * 9,
        out_specs=(P("rep", None, None),) * 9,
        check_vma=False,
    )
```

```python
import functools
import math

import jax
import jax.numpy as jnp
from jax import lax
from jax.experimental import pallas as pl
from jax.experimental.pallas import tpu as pltpu
from jax.sharding import PartitionSpec as P

MESH = pl.DeviceIdType.MESH
F32, BF16 = jnp.float32, jnp.bfloat16
PANELS = 4
LAT = 2
STAGES = 8
G_SLOTS = 2 * LAT + 2
OUT_SLOTS = 4 * LAT + 3
VMEM_LIMIT = 62 * 2**20
PIECE = 4


def dot(a, b):
    return jnp.dot(a, b, preferred_element_type=F32)


def dot_t(a, b):
    return lax.dot_general(a, b, (((1,), (1,)), ((), ())), preferred_element_type=F32)


def scale_of(wide):
    return lax.rsqrt(jnp.mean(wide**2, -1, keepdims=True) + 1e-6)


def normed(h):
    wide = h.astype(F32)
    return (wide * scale_of(wide)).astype(BF16)


def at_rows(start, size):
    return pl.ds(pl.multiple_of(start, size), size)


def forward_kernel(x_ref, wg_ref, wu_ref, wd_ref, h_ref, gu_ref, x_v, a_v, acc, wgu, wdb, gu_v, sem, wsem, gsem):
    tokens = x_v.shape[0]
    panel = wdb.shape[1]
    blocks = wg_ref.shape[2] // panel
    tile = min(512, tokens // 2)

    def weights(b, slot):
        cols = at_rows(b * panel, panel)
        return (
            pltpu.make_async_copy(wg_ref.at[0, :, cols], wgu.at[slot, :, pl.ds(0, panel)], wsem.at[0, slot]),
            pltpu.make_async_copy(wu_ref.at[0, :, cols], wgu.at[slot, :, pl.ds(panel, panel)], wsem.at[1, slot]),
            pltpu.make_async_copy(wd_ref.at[0, cols, :], wdb.at[slot], wsem.at[2, slot]),
        )

    def keep(b, slot):
        return pltpu.make_async_copy(gu_v.at[slot], gu_ref.at[b], gsem.at[slot])

    get = pltpu.make_async_copy(x_ref, x_v, sem)
    get.start()
    for c in weights(0, 0):
        c.start()
    get.wait()

    def norm(t, _):
        rows = at_rows(t * tile, tile)
        a_v[rows, :] = normed(x_v[rows, :])
        acc[rows, :] = jnp.zeros((tile, acc.shape[1]), F32)
        return _

    lax.fori_loop(0, tokens // tile, norm, 0)

    def block(b, carry):
        slot = b % 2

        @pl.when(b + 1 < blocks)
        def _():
            for c in weights(b + 1, 1 - slot):
                c.start()

        for c in weights(b, slot):
            c.wait()

        @pl.when(b >= 2)
        def _():
            keep(b, slot).wait()

        for t in range(tokens // tile):
            rows = pl.ds(t * tile, tile)
            gu = dot(a_v[rows, :], wgu[slot])
            gu_v[slot, rows, :] = gu
            hidden = (jax.nn.silu(gu[:, :panel]) * gu[:, panel:]).astype(BF16)
            acc[rows, :] += dot(hidden, wdb[slot])
        keep(b, slot).start()
        return carry

    lax.fori_loop(0, blocks, block, 0)

    def out(t, _):
        rows = at_rows(t * tile, tile)
        a_v[rows, :] = x_v[rows, :] + acc[rows, :].astype(BF16)
        return _

    lax.fori_loop(0, tokens // tile, out, 0)
    put = pltpu.make_async_copy(a_v, h_ref, sem)
    put.start()
    put.wait()
    for b in range(max(0, blocks - 2), blocks):
        keep(b, b % 2).wait()


def forward(x, wg, wu, wd):
    tokens, d = x.shape
    panel = d // PANELS
    blocks = wg.shape[2] // panel
    hbm = pl.BlockSpec(memory_space=pl.ANY)
    return pl.pallas_call(
        forward_kernel,
        out_shape=(jax.ShapeDtypeStruct(x.shape, BF16), jax.ShapeDtypeStruct((blocks, tokens, 2 * panel), F32)),
        in_specs=[hbm] * 4,
        out_specs=(hbm, hbm),
        scratch_shapes=[
            pltpu.VMEM((tokens, d), BF16),
            pltpu.VMEM((tokens, d), BF16),
            pltpu.VMEM((tokens, d), F32),
            pltpu.VMEM((2, d, 2 * panel), BF16),
            pltpu.VMEM((2, panel, d), BF16),
            pltpu.VMEM((2, tokens, 2 * panel), F32),
            pltpu.SemaphoreType.DMA,
            pltpu.SemaphoreType.DMA((3, 2)),
            pltpu.SemaphoreType.DMA((2,)),
        ],
        compiler_params=pltpu.CompilerParams(vmem_limit_bytes=VMEM_LIMIT),
        cost_estimate=pl.CostEstimate(flops=6 * tokens * d * wg.shape[2], bytes_accessed=2 * (2 * x.size + 3 * d * wg.shape[2]), transcendentals=tokens * wg.shape[2]),
        name="forward",
    )(x, wg, wu, wd)


def backward_kernel(side, x_ref, h_ref, kept_ref, dy_ref, wg_ref, wu_ref, wd_ref, g_ref, *refs):
    later_q, first_q, refs = refs[0:4], refs[4:8], refs[8:]
    a_v, at_v, ct_v, acc, wgu, wdb, hidt, dgu, own, part1, done, sbuf, rbuf, sem, wsem, osem, ssem, rsem = refs
    tokens, d = a_v.shape
    panel = wdb.shape[1]
    blocks = wg_ref.shape[2] // panel
    quarter, unit = panel // side, panel // side // side
    tile = min(512, tokens // 4)
    first, chunks = blocks * 3, 2 * blocks * 3
    half = 3 * quarter + 3 * unit
    X1, X2, Y1, Y2 = 0, quarter, 3 * quarter, 3 * quarter + unit
    AY1, AY2, AX1, AX2 = half, half + 2 * unit, half + 3 * unit, half + 3 * unit + 2 * quarter

    rep, me = lax.axis_index("rep"), lax.axis_index("dp")
    px, py = me // side, me % side
    device = lambda x, y: (rep, (x % side) * side + y % side)
    near = (device(px + 1, py), device(px + side - 1, py), device(px, py + 1), device(px, py + side - 1))
    colours = ((0, (0, 1), (2, 3), px, py), (1, (2, 3), (0, 1), py, px))

    barrier = pltpu.get_barrier_semaphore()
    for n in near:
        pl.semaphore_signal(barrier, inc=1, device_id=n, device_id_type=MESH)
    pl.semaphore_wait(barrier, 4)

    parts = ((X1, Y1), (Y1, AX1), (AX1, AX2), (AX2, 2 * half))
    sent_in = ((0, chunks + LAT), (2 * LAT, chunks + 5 * LAT), (6 * LAT, first + 6 * LAT), (7 * LAT, first + 7 * LAT))

    def parts_of(k):
        return [which for which in range(4) if which < 2 or (k - (which + 4) * LAT) % 3 == 0]


    def message(link, which, i):
        rows = pl.ds(parts[which][0], parts[which][1] - parts[which][0])
        return pltpu.make_async_remote_copy(
            src_ref=sbuf.at[link, i % LAT, rows],
            dst_ref=rbuf.at[link, i % (2 * LAT), rows],
            send_sem=ssem.at[which, link, i % LAT],
            recv_sem=rsem.at[which, link, i % (2 * LAT)],
            device_id=near[link],
            device_id_type=MESH,
        )

    def take_whole(c):
        pltpu.make_async_copy(done.at[c % OUT_SLOTS], g_ref.at[c // 3], osem.at[c % OUT_SLOTS]).start()

    def take_quarters(k, c, refs):
        slot = c % OUT_SLOTS
        for colour, _, _, p, _ in colours:
            for j in range(2):
                rows = at_rows((2 * colour + j) * panel + p * quarter, quarter)
                to = refs[2 * colour + j].at[k, (c // 3) % blocks]
                pltpu.make_async_copy(done.at[slot, rows], to, osem.at[slot]).start()

    def wait_whole(c):
        pltpu.make_async_copy(done.at[c % OUT_SLOTS], g_ref.at[0], osem.at[c % OUT_SLOTS]).wait()

    def wait_quarters(c):
        rows = pl.ds(0, quarter)
        for _ in range(PANELS):
            pltpu.make_async_copy(done.at[c % OUT_SLOTS, rows], first_q[0].at[0, 0], osem.at[c % OUT_SLOTS]).wait()

    def tick(i, k):
        sent, got = i % LAT, (i + LAT) % (2 * LAT)

        for which in parts_of((k - LAT) % 3):
            start, stop = sent_in[which]

            @pl.when((i >= start + LAT) & (i < stop + LAT))
            def _(which=which):
                for link in range(4):
                    message(link, which, i + LAT).wait_send()
                    message(link, which, i + LAT).wait_recv()

        def stage(s, stop=chunks):
            c = i - s * LAT
            return c, pl.when((c >= 0) & (c < stop))

        def quarter_rows(p, k):
            return at_rows(p * panel + (k % side) * quarter, quarter)

        def unit_rows(p, k, j):
            return at_rows(p * panel + (k % side) * quarter + (j % side) * unit, unit)

        def unit_of(p, j):
            return at_rows(p * quarter + (j % side) * unit, unit)

        wide = lambda v: v.astype(F32)

        c0, when = stage(0)

        @when
        def _():
            for colour, one, two, p, q in colours:
                for j in range(2):
                    sbuf[one[j], sent, pl.ds(X1, quarter)] = own[c0 % G_SLOTS, quarter_rows(2 * colour + j, p + 2)]

        c1, when = stage(1)

        @when
        def _():
            slot = c1 % G_SLOTS
            for colour, one, two, p, q in colours:
                for j in range(2):
                    to = p + (1, side - 1)[j]
                    for w in range(2):
                        v = own[slot, quarter_rows(2 * colour + w, to)]
                        if w == j:
                            v = (wide(v) + wide(rbuf[one[j], got, pl.ds(X1, quarter)])).astype(BF16)
                        sbuf[one[j], sent, pl.ds(X2 + w * quarter, quarter)] = v

        c2, when = stage(2)

        @when
        def _():
            slot = c2 % G_SLOTS
            for colour, one, two, p, q in colours:
                for w in range(2):
                    rows = pl.ds(X2 + w * quarter, quarter)
                    part1[slot, colour, pl.ds(w * quarter, quarter)] = (
                        wide(own[slot, quarter_rows(2 * colour + w, p)]) + wide(rbuf[one[0], got, rows]) + wide(rbuf[one[1], got, rows])
                    )
                for j in range(2):
                    sbuf[two[j], sent, pl.ds(Y1, unit)] = part1[slot, colour, unit_of(j, q + 2)].astype(BF16)

        c3, when = stage(3)

        @when
        def _():
            slot = c3 % G_SLOTS
            for colour, one, two, p, q in colours:
                for j in range(2):
                    to = q + (1, side - 1)[j]
                    for w in range(2):
                        v = part1[slot, colour, unit_of(w, to)]
                        if w == j:
                            v = v + wide(rbuf[two[j], got, pl.ds(Y1, unit)])
                        sbuf[two[j], sent, pl.ds(Y2 + w * unit, unit)] = v.astype(BF16)

        c4, when = stage(4)

        @when
        def _():
            if (k - 4 * LAT - OUT_SLOTS) % 3 == 0:

                @pl.when((c4 >= OUT_SLOTS) & (c4 < first + OUT_SLOTS))
                def _():
                    wait_whole(c4)

                pl.when(c4 >= first + OUT_SLOTS)(lambda: wait_quarters(c4))
            else:
                pl.when(c4 >= OUT_SLOTS)(lambda: wait_quarters(c4))

            slot, to = c4 % G_SLOTS, c4 % OUT_SLOTS
            for colour, one, two, p, q in colours:
                for w in range(2):
                    rows = pl.ds(Y2 + w * unit, unit)
                    v = part1[slot, colour, unit_of(w, q)] + wide(rbuf[two[0], got, rows]) + wide(rbuf[two[1], got, rows])
                    v = v.astype(BF16)
                    done[to, unit_rows(2 * colour + w, p, q)] = v
                    for j in range(2):
                        sbuf[two[j], sent, pl.ds(AY1 + w * unit, unit)] = v

        c5, when = stage(5)

        @when
        def _():
            to = c5 % OUT_SLOTS
            for colour, one, two, p, q in colours:
                for j in range(2):
                    for w in range(2):
                        v = rbuf[two[j], got, pl.ds(AY1 + w * unit, unit)]
                        done[to, unit_rows(2 * colour + w, p, q + (side - 1, 1)[j])] = v
                        if w == j:
                            sbuf[two[j], sent, pl.ds(AY2, unit)] = v

        c6, when = stage(6)

        @when
        def _():
            to = c6 % OUT_SLOTS
            for colour, one, two, p, q in colours:
                for j in range(2):
                    done[to, unit_rows(2 * colour + j, p, q + 2)] = rbuf[two[j], got, pl.ds(AY2, unit)]

            kind = (k - 6 * LAT) % 3

            @pl.when(c6 < first)
            def _():
                if kind:
                    take_quarters(kind - 1, c6, later_q)
                else:
                    for colour, one, two, p, q in colours:
                        for w in range(2):
                            v = done[to, quarter_rows(2 * colour + w, p)]
                            for j in range(2):
                                sbuf[one[j], sent, pl.ds(AX1 + w * quarter, quarter)] = v

            pl.when(c6 >= first)(lambda: take_quarters(kind, c6, first_q))

        c7, when = stage(7, first)

        def spread():
            to = c7 % OUT_SLOTS
            for colour, one, two, p, q in colours:
                for j in range(2):
                    for w in range(2):
                        v = rbuf[one[j], got, pl.ds(AX1 + w * quarter, quarter)]
                        done[to, quarter_rows(2 * colour + w, p + (side - 1, 1)[j])] = v
                        if w == j:
                            sbuf[one[j], sent, pl.ds(AX2, quarter)] = v

        if (k - 7 * LAT) % 3 == 0:
            when(spread)

        c8, when = stage(8, first)

        def finish():
            to = c8 % OUT_SLOTS
            for colour, one, two, p, q in colours:
                for j in range(2):
                    done[to, quarter_rows(2 * colour + j, p + 2)] = rbuf[one[j], got, pl.ds(AX2, quarter)]
            take_whole(c8)

        if (k - 8 * LAT) % 3 == 0:
            when(finish)

        for which in parts_of(k):
            start, stop = sent_in[which]

            @pl.when((i >= start) & (i < stop))
            def _(which=which):
                for link in range(4):
                    message(link, which, i).start()

    def weights(number, slot):
        layer, cols = 1 - number // blocks, at_rows((number % blocks) * panel, panel)
        return (
            pltpu.make_async_copy(wg_ref.at[layer, :, cols], wgu.at[slot, :, pl.ds(0, panel)], wsem.at[0, slot]),
            pltpu.make_async_copy(wu_ref.at[layer, :, cols], wgu.at[slot, :, pl.ds(panel, panel)], wsem.at[1, slot]),
            pltpu.make_async_copy(wd_ref.at[layer, cols, :], wdb.at[slot], wsem.at[2, slot]),
        )

    def take_in(_t, _):
        rows = at_rows(_t * tile, tile)
        a = normed(a_v[rows, :])
        a_v[rows, :] = a
        at_v[:, rows] = a.T
        return _

    def columns_of(number):
        return at_rows((number % 2) * 2 * panel, 2 * panel)

    def fetch(number):
        return pltpu.make_async_copy(kept_ref.at[number - blocks], acc.at[:, columns_of(number)], sem.at[number % 2])

    for c in weights(0, 0):
        c.start()
    gets = (pltpu.make_async_copy(h_ref, a_v, sem.at[0]), pltpu.make_async_copy(dy_ref, ct_v, sem.at[1]))
    for c in gets:
        c.start()
    for c in gets:
        c.wait()
    lax.fori_loop(0, tokens // tile, take_in, 0)

    def next_layer():
        get = pltpu.make_async_copy(h_ref, a_v, sem.at[0])
        get.start()
        get.wait()
        small = tile // 4

        def back(t, _):
            rows = at_rows(t * small, small)
            wide = a_v[rows, :].astype(F32)
            scale = scale_of(wide)
            by_a = acc[rows, :].astype(BF16).astype(F32)
            inner = jnp.mean(by_a * wide, -1, keepdims=True)
            by_h = by_a * scale - wide * (scale * scale * scale * inner)
            ct_v[rows, :] = ct_v[rows, :] + by_h.astype(BF16)
            return _

        lax.fori_loop(0, tokens // small, back, 0)
        get = pltpu.make_async_copy(x_ref, a_v, sem.at[0])
        get.start()
        get.wait()
        fetch(blocks).start()
        lax.fori_loop(0, tokens // tile, take_in, 0)

    def block(number, carry):
        slot = number % 2
        later = number < blocks
        i = 3 * number

        pl.when(number == blocks)(next_layer)

        for c in weights(number, slot):
            c.wait()

        @pl.when(number + 1 < 2 * blocks)
        def _():
            for c in weights(number + 1, 1 - slot):
                c.start()

        @pl.when(number >= blocks)
        def _():
            pltpu.make_async_copy(kept_ref.at[0], acc.at[:, columns_of(number)], sem.at[slot]).wait()

            @pl.when(number + 1 < 2 * blocks)
            def _():
                fetch(number + 1).start()

        def hidden(t, gu):
            rows = pl.ds(t * tile, tile)
            by_hidden = dot_t(ct_v[rows, :], wdb[slot]).astype(BF16).astype(F32)
            gate, up = gu[:, :panel], gu[:, panel:]
            sigmoid = jax.nn.sigmoid(gate)
            silu = gate * sigmoid
            hidt[:, rows] = (silu * up).astype(BF16).T
            dgu[rows, pl.ds(0, panel)] = (by_hidden * up * (sigmoid + silu * (1.0 - sigmoid))).astype(BF16)
            dgu[rows, pl.ds(panel, panel)] = (by_hidden * silu).astype(BF16)

        def hidden_half(part):
            tiles = tokens // tile // 2

            @pl.when(later)
            def _():
                for t in range(part * tiles, part * tiles + tiles):
                    hidden(t, dot(a_v[pl.ds(t * tile, tile), :], wgu[slot]))

            @pl.when(number >= blocks)
            def _():
                for t in range(part * tiles, part * tiles + tiles):
                    hidden(t, acc[pl.ds(t * tile, tile), columns_of(number)])

        hidden_half(0)

        @pl.when(number > 0)
        def _():
            tick(i - 1, 2)

        hidden_half(1)
        for k in range(PANELS):
            own[i % G_SLOTS, pl.ds(k * panel, panel)] = dot(hidt[...], ct_v[:, pl.ds(k * panel, panel)]).astype(BF16)
        tick(i, 0)
        for k in range(PANELS):
            v = dot(at_v[pl.ds(k * panel, panel), :], dgu[...]).astype(BF16)
            own[(i + 1) % G_SLOTS, pl.ds(k * panel, panel)] = v[:, :panel]
            own[(i + 2) % G_SLOTS, pl.ds(k * panel, panel)] = v[:, panel:]
        tick(i + 1, 1)

        @pl.when(later)
        def _():
            for t in range(tokens // tile):
                rows = pl.ds(t * tile, tile)
                v = dot_t(dgu[rows, :], wgu[slot])
                acc[rows, :] = jnp.where(number == 0, v, acc[rows, :] + v)

        return carry

    lax.fori_loop(0, 2 * blocks, block, 0)

    tick(chunks - 1, 2)

    def drain(t, _):
        for k in range(3):
            tick(chunks + 3 * t + k, k)
        return _

    lax.fori_loop(0, (6 * LAT + 2) // 3, drain, 0)
    for c in range(chunks - OUT_SLOTS, chunks):
        (wait_whole if c < first and c % 3 == 0 else wait_quarters)(c)


def backward(side, x, h, kept, dy, wg, wu, wd):
    tokens, d = x.shape
    panel = d // PANELS
    blocks = wg.shape[2] // panel
    rows = 6 * (panel // side + panel // side // side)
    hbm = pl.BlockSpec(memory_space=pl.ANY)
    return pl.pallas_call(
        functools.partial(backward_kernel, side),
        out_shape=(jax.ShapeDtypeStruct((blocks, d, panel), BF16),)
        + tuple(jax.ShapeDtypeStruct((n, blocks, panel // side, panel), BF16) for n in (2, 3) for _ in range(PANELS)),
        in_specs=[hbm] * 7,
        out_specs=(hbm,) * 9,
        scratch_shapes=[
            pltpu.VMEM((tokens, d), BF16),
            pltpu.VMEM((d, tokens), BF16),
            pltpu.VMEM((tokens, d), BF16),
            pltpu.VMEM((tokens, d), F32),
            pltpu.VMEM((2, d, 2 * panel), BF16),
            pltpu.VMEM((2, panel, d), BF16),
            pltpu.VMEM((panel, tokens), BF16),
            pltpu.VMEM((tokens, 2 * panel), BF16),
            pltpu.VMEM((G_SLOTS, d, panel), BF16),
            pltpu.VMEM((G_SLOTS, 2, 2 * panel // side, panel), F32),
            pltpu.VMEM((OUT_SLOTS, d, panel), BF16),
            pltpu.VMEM((4, LAT, rows, panel), BF16),
            pltpu.VMEM((4, 2 * LAT, rows, panel), BF16),
            pltpu.SemaphoreType.DMA((2,)),
            pltpu.SemaphoreType.DMA((3, 2)),
            pltpu.SemaphoreType.DMA((OUT_SLOTS,)),
            pltpu.SemaphoreType.DMA((4, 4, LAT)),
            pltpu.SemaphoreType.DMA((4, 4, 2 * LAT)),
        ],
        compiler_params=pltpu.CompilerParams(collective_id=0, has_side_effects=True, vmem_limit_bytes=VMEM_LIMIT),
        cost_estimate=pl.CostEstimate(flops=24 * tokens * d * wg.shape[2], bytes_accessed=4 * 3 * wg.size, transcendentals=2 * tokens * wg.shape[2]),
        name="backward",
    )(x, h, kept, dy, wg, wu, wd)


def adamw(w, m, v, g):
    m = 0.9 * m + 0.1 * g
    v = 0.95 * v + 0.05 * g * g
    step = m * lax.rsqrt(v + 1e-8) + 0.1 * w
    return (w - 0.02 * step).astype(BF16), m, v


RING = 10
AHEAD = 6


def update_kernel(side, plan, sources, fresh, *refs):
    wmv, refs = (refs[0:3], refs[3:6], refs[6:9]), refs[9:]
    source, refs = refs[:sources], refs[sources:]
    refs = refs if fresh else refs[9:]
    new, refs = (refs[0:3], refs[3:6], refs[6:9]), refs[9:]
    tall, flat, gbuf, isem, osem = refs[0:3], refs[3:6], refs[6], refs[7], refs[8]
    _, quarter, panel = gbuf.shape[2:]
    me = lax.axis_index("dp")
    position = (me // side, me % side)
    units = plan

    def arrays(refs, u):
        layer, kind, start, blocks, colour, k, relative, _ = units[u]
        k = (position[colour] + k + side) % side if relative else k
        if kind == 0:
            at = (layer, pl.ds(start, blocks), k, slice(None), pl.ds(2 * colour * panel, 2 * panel))
        else:
            at = (layer, pl.ds(2 * colour, 2), k, slice(None), pl.ds(start * panel, blocks * panel))
        return [r[(2, 0, 1)[kind]].at[at] for r in refs]

    def buffers(u):
        blocks = units[u][3]
        if units[u][1] == 0:
            return [b.at[u % RING, pl.ds(0, blocks)] for b in flat]
        return [b.at[u % RING, :, :, pl.ds(0, blocks * panel)] for b in tall]

    def copies_in(u):
        _, _, start, blocks, _, _, _, halves = units[u]
        slot = u % RING
        cs = [pltpu.make_async_copy(a, b, isem.at[n, slot]) for n, (a, b) in enumerate(zip(arrays(wmv, u), buffers(u)))]
        for j, (which, index, rows) in enumerate(halves):
            ref = source[which] if index is None else source[which].at[index]
            ref = ref.at[pl.ds(start, blocks), pl.ds(rows, quarter)]
            cs.append(pltpu.make_async_copy(ref, gbuf.at[slot, j, pl.ds(0, blocks)], isem.at[3 + j, slot]))
        return cs

    def copies_out(u):
        return [pltpu.make_async_copy(b, a, osem.at[n, u % RING]) for n, (a, b) in enumerate(zip(arrays(new, u), buffers(u)))]

    def begin(u):
        for c in copies_in(u):
            c.start()

    for u in range(min(AHEAD, len(units))):
        begin(u)
    for u in range(len(units)):
        if u + AHEAD < len(units):
            if u + AHEAD >= RING:
                for c in copies_out(u + AHEAD - RING):
                    c.wait()
            begin(u + AHEAD)
        for c in copies_in(u):
            c.wait()
        slot = u % RING
        w_b, m_b, v_b = flat if units[u][1] == 0 else tall

        def part(b, carry):
            for j in range(2):
                if units[u][1] == 0:
                    at = (slot, b, slice(None), pl.ds(j * panel, panel))
                else:
                    at = (slot, j, slice(None), at_rows(b * panel, panel))
                w_b[at], m_b[at], v_b[at] = adamw(w_b[at].astype(F32), m_b[at], v_b[at], gbuf[slot, j, b].astype(F32))
            return carry

        lax.fori_loop(0, units[u][3], part, 0)
        for c in copies_out(u):
            c.start()
    for u in range(max(0, len(units) - RING), len(units)):
        for c in copies_out(u):
            c.wait()


def update(side, plan, wmv, sources, old):
    _, _, _, quarter, ff = wmv[0].shape
    blocks = max(one[3] for one in plan)
    panel = ff // wmv[2].shape[1]
    hbm = pl.BlockSpec(memory_space=pl.ANY)
    size = sum(one[3] for one in plan) * 2 * quarter * panel
    return pl.pallas_call(
        functools.partial(update_kernel, side, plan, len(sources), old is None),
        out_shape=tuple(jax.ShapeDtypeStruct(a.shape, a.dtype) for a in wmv),
        in_specs=[hbm] * (9 + len(sources) + (0 if old is None else 9)),
        out_specs=(hbm,) * 9,
        input_output_aliases={} if old is None else {9 + len(sources) + n: n for n in range(9)},
        scratch_shapes=[pltpu.VMEM((RING, 2, quarter, blocks * panel), t) for t in (BF16, F32, F32)]
        + [pltpu.VMEM((RING, blocks, quarter, 2 * panel), t) for t in (BF16, F32, F32)]
        + [pltpu.VMEM((RING, 2, blocks, quarter, panel), BF16), pltpu.SemaphoreType.DMA((5, RING)), pltpu.SemaphoreType.DMA((3, RING))],
        compiler_params=pltpu.CompilerParams(vmem_limit_bytes=VMEM_LIMIT),
        cost_estimate=pl.CostEstimate(flops=size * 6000, bytes_accessed=22 * size, transcendentals=size),
        name="update",
    )(*wmv, *sources, *(old or ()))


def solution(mesh):
    side = math.isqrt(mesh.shape["dp"])
    spots = [(x, y) for x in range(side) for y in range(side)]

    def shift(dx, dy):
        return [(x * side + y, (x + dx) % side * side + (y + dy) % side) for x, y in spots]

    ways = ((shift(1, 0), shift(-1, 0)), (shift(0, 1), shift(0, -1)))

    def step(x, dy, *arrays):
        weights = arrays[:3]
        x, dy = x[0], dy[0]
        d, ff = weights[0].shape[1:]
        panel = d // PANELS
        quarter, blocks = panel // side, ff // panel
        h, kept = forward(x, *weights)
        whole, *quarters = backward(side, x, h, kept, dy, *weights)
        wmv = [a.reshape(a.shape[0], blocks, side, quarter, d) if n % 3 == 2 else a.reshape(a.shape[0], PANELS, side, quarter, ff) for n, a in enumerate(arrays)]

        def near(quarters):
            return [lax.ppermute(q, "dp", ways[n // 2][way]) for way in range(2) for n, q in enumerate(quarters)]

        def far(near):
            return [lax.ppermute(near[4 * (n % 2) + n], "dp", ways[n // 2][n % 2]) for n in range(4)]

        def pieces(layer, kinds, colour, k, relative, halves):
            return [
                (layer, kind, start, min(PIECE, blocks - start), colour, k, relative, halves(kind)) for kind in kinds for start in range(0, blocks, PIECE)
            ]

        def join(parts):
            return [one for part in parts for one in part]

        def three(layer, kinds):
            return join(
                pieces(layer, kinds, c, r, True, lambda kind: [(4 * s + 2 * c + j, kind - kinds[0], 0) for j in range(2)])
                for c in range(2)
                for s, r in enumerate((0, -1, 1))
            )

        def last(layer, kinds, at):
            return join(pieces(layer, kinds, c, 2, True, lambda kind: [(at + 2 * c + j, kind - kinds[0], 0) for j in range(2)]) for c in range(2))

        def known(layer, kind):
            return join(
                pieces(layer, (kind,), c, k, False, lambda _: [(0, None, (2 * c + j) * panel + k * quarter) for j in range(2)])
                for c in range(2)
                for k in range(side)
            )

        later, first = quarters[:4], quarters[4:]
        later_near, first_near = near(later), near(first)
        new = update(side, known(1, 0), wmv, [whole], None)
        later_far = far(later_near)
        new = update(side, three(1, (1, 2)), wmv, [*later, *later_near], new)
        first_far = far(first_near)
        new = update(side, three(0, (0, 1, 2)), wmv, [*first, *first_near], new)
        new = update(side, last(1, (1, 2), 0) + last(0, (0, 1, 2), 4), wmv, [*later_far, *first_far], new)
        return tuple(a.reshape(b.shape) for a, b in zip(new, arrays, strict=True))

    return jax.shard_map(
        step,
        mesh=mesh,
        in_specs=(P(("rep", "dp"), None, None),) * 2 + (P(None, None, None),) * 9,
        out_specs=(P("rep", None, None),) * 9,
        check_vma=False,
    )
```

```python
import functools
import math

import jax
import jax.numpy as jnp
from jax import lax
from jax.experimental import pallas as pl
from jax.experimental.pallas import tpu as pltpu
from jax.sharding import PartitionSpec as P

MESH = pl.DeviceIdType.MESH
F32, BF16 = jnp.float32, jnp.bfloat16
PANELS = 4
LAT = 2
STAGES = 8
G_SLOTS = 2 * LAT + 2
OUT_SLOTS = 4 * LAT + 3
VMEM_LIMIT = 62 * 2**20


def dot(a, b):
    return jnp.dot(a, b, preferred_element_type=F32)


def dot_t(a, b):
    return lax.dot_general(a, b, (((1,), (1,)), ((), ())), preferred_element_type=F32)


def scale_of(wide):
    return lax.rsqrt(jnp.mean(wide**2, -1, keepdims=True) + 1e-6)


def normed(h):
    wide = h.astype(F32)
    return (wide * scale_of(wide)).astype(BF16)


def at_rows(start, size):
    return pl.ds(pl.multiple_of(start, size), size)


def forward_kernel(x_ref, wg_ref, wu_ref, wd_ref, h_ref, gu_ref, x_v, a_v, acc, wgu, wdb, gu_v, sem, wsem, gsem):
    tokens = x_v.shape[0]
    panel = wdb.shape[1]
    blocks = wg_ref.shape[2] // panel
    tile = min(512, tokens // 2)

    def weights(b, slot):
        cols = at_rows(b * panel, panel)
        return (
            pltpu.make_async_copy(wg_ref.at[0, :, cols], wgu.at[slot, :, pl.ds(0, panel)], wsem.at[0, slot]),
            pltpu.make_async_copy(wu_ref.at[0, :, cols], wgu.at[slot, :, pl.ds(panel, panel)], wsem.at[1, slot]),
            pltpu.make_async_copy(wd_ref.at[0, cols, :], wdb.at[slot], wsem.at[2, slot]),
        )

    def keep(b, slot):
        return pltpu.make_async_copy(gu_v.at[slot], gu_ref.at[b], gsem.at[slot])

    get = pltpu.make_async_copy(x_ref, x_v, sem)
    get.start()
    for c in weights(0, 0):
        c.start()
    get.wait()

    def norm(t, _):
        rows = at_rows(t * tile, tile)
        a_v[rows, :] = normed(x_v[rows, :])
        acc[rows, :] = jnp.zeros((tile, acc.shape[1]), F32)
        return _

    lax.fori_loop(0, tokens // tile, norm, 0)

    def block(b, carry):
        slot = b % 2

        @pl.when(b + 1 < blocks)
        def _():
            for c in weights(b + 1, 1 - slot):
                c.start()

        for c in weights(b, slot):
            c.wait()

        @pl.when(b >= 2)
        def _():
            keep(b, slot).wait()

        for t in range(tokens // tile):
            rows = pl.ds(t * tile, tile)
            gu = dot(a_v[rows, :], wgu[slot])
            gu_v[slot, rows, :] = gu
            hidden = (jax.nn.silu(gu[:, :panel]) * gu[:, panel:]).astype(BF16)
            acc[rows, :] += dot(hidden, wdb[slot])
        keep(b, slot).start()
        return carry

    lax.fori_loop(0, blocks, block, 0)

    def out(t, _):
        rows = at_rows(t * tile, tile)
        a_v[rows, :] = x_v[rows, :] + acc[rows, :].astype(BF16)
        return _

    lax.fori_loop(0, tokens // tile, out, 0)
    put = pltpu.make_async_copy(a_v, h_ref, sem)
    put.start()
    put.wait()
    for b in range(max(0, blocks - 2), blocks):
        keep(b, b % 2).wait()


def forward(x, wg, wu, wd):
    tokens, d = x.shape
    panel = d // PANELS
    blocks = wg.shape[2] // panel
    hbm = pl.BlockSpec(memory_space=pl.ANY)
    return pl.pallas_call(
        forward_kernel,
        out_shape=(jax.ShapeDtypeStruct(x.shape, BF16), jax.ShapeDtypeStruct((blocks, tokens, 2 * panel), F32)),
        in_specs=[hbm] * 4,
        out_specs=(hbm, hbm),
        scratch_shapes=[
            pltpu.VMEM((tokens, d), BF16),
            pltpu.VMEM((tokens, d), BF16),
            pltpu.VMEM((tokens, d), F32),
            pltpu.VMEM((2, d, 2 * panel), BF16),
            pltpu.VMEM((2, panel, d), BF16),
            pltpu.VMEM((2, tokens, 2 * panel), F32),
            pltpu.SemaphoreType.DMA,
            pltpu.SemaphoreType.DMA((3, 2)),
            pltpu.SemaphoreType.DMA((2,)),
        ],
        compiler_params=pltpu.CompilerParams(vmem_limit_bytes=VMEM_LIMIT),
        cost_estimate=pl.CostEstimate(flops=6 * tokens * d * wg.shape[2], bytes_accessed=2 * (2 * x.size + 3 * d * wg.shape[2]), transcendentals=tokens * wg.shape[2]),
        name="forward",
    )(x, wg, wu, wd)


def backward_kernel(side, x_ref, h_ref, kept_ref, dy_ref, wg_ref, wu_ref, wd_ref, g_ref, *refs):
    later_q, first_q, refs = refs[0:2], refs[2:4], refs[4:]
    a_v, at_v, ct_v, acc, wgu, wdb, hidt, dgu, own, part1, done, sbuf, rbuf, sem, wsem, osem, ssem, rsem = refs
    tokens, d = a_v.shape
    panel = wdb.shape[1]
    blocks = wg_ref.shape[2] // panel
    quarter, unit = panel // side, panel // side // side
    tile = min(512, tokens // 4)
    first, chunks = blocks * 3, 2 * blocks * 3
    half = 3 * quarter + 3 * unit
    X1, X2, Y1, Y2 = 0, quarter, 3 * quarter, 3 * quarter + unit
    AY1, AY2, AX1, AX2 = half, half + 2 * unit, half + 3 * unit, half + 3 * unit + 2 * quarter

    rep, me = lax.axis_index("rep"), lax.axis_index("dp")
    px, py = me // side, me % side
    device = lambda x, y: (rep, (x % side) * side + y % side)
    near = (device(px + 1, py), device(px + side - 1, py), device(px, py + 1), device(px, py + side - 1))
    colours = ((0, (0, 1), (2, 3), px, py), (1, (2, 3), (0, 1), py, px))

    barrier = pltpu.get_barrier_semaphore()
    for n in near:
        pl.semaphore_signal(barrier, inc=1, device_id=n, device_id_type=MESH)
    pl.semaphore_wait(barrier, 4)

    parts = ((X1, Y1), (Y1, AX1), (AX1, AX2), (AX2, 2 * half))
    sent_in = ((0, chunks + LAT), (2 * LAT, chunks + 5 * LAT), (6 * LAT, first + 6 * LAT), (7 * LAT, first + 7 * LAT))

    def parts_of(k):
        return [which for which in range(4) if which < 2 or (k - (which + 4) * LAT) % 3 == 0]


    def message(link, which, i):
        rows = pl.ds(parts[which][0], parts[which][1] - parts[which][0])
        return pltpu.make_async_remote_copy(
            src_ref=sbuf.at[link, i % LAT, rows],
            dst_ref=rbuf.at[link, i % (2 * LAT), rows],
            send_sem=ssem.at[which, link, i % LAT],
            recv_sem=rsem.at[which, link, i % (2 * LAT)],
            device_id=near[link],
            device_id_type=MESH,
        )

    def take_whole(c):
        pltpu.make_async_copy(done.at[c % OUT_SLOTS], g_ref.at[c // 3], osem.at[c % OUT_SLOTS]).start()

    def take_quarters(k, c, refs):
        slot = c % OUT_SLOTS
        for colour, _, _, p, _ in colours:
            for j in range(2):
                rows = at_rows((2 * colour + j) * panel + p * quarter, quarter)
                to = refs[colour].at[j, k, (c // 3) % blocks]
                pltpu.make_async_copy(done.at[slot, rows], to, osem.at[slot]).start()

    def wait_whole(c):
        pltpu.make_async_copy(done.at[c % OUT_SLOTS], g_ref.at[0], osem.at[c % OUT_SLOTS]).wait()

    def wait_quarters(c):
        rows = pl.ds(0, quarter)
        for _ in range(PANELS):
            pltpu.make_async_copy(done.at[c % OUT_SLOTS, rows], first_q[0].at[0, 0, 0], osem.at[c % OUT_SLOTS]).wait()

    def tick(i, k):
        sent, got = i % LAT, (i + LAT) % (2 * LAT)

        for which in parts_of((k - LAT) % 3):
            start, stop = sent_in[which]

            @pl.when((i >= start + LAT) & (i < stop + LAT))
            def _(which=which):
                for link in range(4):
                    message(link, which, i + LAT).wait_send()
                    message(link, which, i + LAT).wait_recv()

        def stage(s, stop=chunks):
            c = i - s * LAT
            return c, pl.when((c >= 0) & (c < stop))

        def quarter_rows(p, k):
            return at_rows(p * panel + (k % side) * quarter, quarter)

        def unit_rows(p, k, j):
            return at_rows(p * panel + (k % side) * quarter + (j % side) * unit, unit)

        def unit_of(p, j):
            return at_rows(p * quarter + (j % side) * unit, unit)

        wide = lambda v: v.astype(F32)

        c0, when = stage(0)

        @when
        def _():
            for colour, one, two, p, q in colours:
                for j in range(2):
                    sbuf[one[j], sent, pl.ds(X1, quarter)] = own[c0 % G_SLOTS, quarter_rows(2 * colour + j, p + 2)]

        c1, when = stage(1)

        @when
        def _():
            slot = c1 % G_SLOTS
            for colour, one, two, p, q in colours:
                for j in range(2):
                    to = p + (1, side - 1)[j]
                    for w in range(2):
                        v = own[slot, quarter_rows(2 * colour + w, to)]
                        if w == j:
                            v = (wide(v) + wide(rbuf[one[j], got, pl.ds(X1, quarter)])).astype(BF16)
                        sbuf[one[j], sent, pl.ds(X2 + w * quarter, quarter)] = v

        c2, when = stage(2)

        @when
        def _():
            slot = c2 % G_SLOTS
            for colour, one, two, p, q in colours:
                for w in range(2):
                    rows = pl.ds(X2 + w * quarter, quarter)
                    part1[slot, colour, pl.ds(w * quarter, quarter)] = (
                        wide(own[slot, quarter_rows(2 * colour + w, p)]) + wide(rbuf[one[0], got, rows]) + wide(rbuf[one[1], got, rows])
                    )
                for j in range(2):
                    sbuf[two[j], sent, pl.ds(Y1, unit)] = part1[slot, colour, unit_of(j, q + 2)].astype(BF16)

        c3, when = stage(3)

        @when
        def _():
            slot = c3 % G_SLOTS
            for colour, one, two, p, q in colours:
                for j in range(2):
                    to = q + (1, side - 1)[j]
                    for w in range(2):
                        v = part1[slot, colour, unit_of(w, to)]
                        if w == j:
                            v = v + wide(rbuf[two[j], got, pl.ds(Y1, unit)])
                        sbuf[two[j], sent, pl.ds(Y2 + w * unit, unit)] = v.astype(BF16)

        c4, when = stage(4)

        @when
        def _():
            if (k - 4 * LAT - OUT_SLOTS) % 3 == 0:

                @pl.when((c4 >= OUT_SLOTS) & (c4 < first + OUT_SLOTS))
                def _():
                    wait_whole(c4)

                pl.when(c4 >= first + OUT_SLOTS)(lambda: wait_quarters(c4))
            else:
                pl.when(c4 >= OUT_SLOTS)(lambda: wait_quarters(c4))

            slot, to = c4 % G_SLOTS, c4 % OUT_SLOTS
            for colour, one, two, p, q in colours:
                for w in range(2):
                    rows = pl.ds(Y2 + w * unit, unit)
                    v = part1[slot, colour, unit_of(w, q)] + wide(rbuf[two[0], got, rows]) + wide(rbuf[two[1], got, rows])
                    v = v.astype(BF16)
                    done[to, unit_rows(2 * colour + w, p, q)] = v
                    for j in range(2):
                        sbuf[two[j], sent, pl.ds(AY1 + w * unit, unit)] = v

        c5, when = stage(5)

        @when
        def _():
            to = c5 % OUT_SLOTS
            for colour, one, two, p, q in colours:
                for j in range(2):
                    for w in range(2):
                        v = rbuf[two[j], got, pl.ds(AY1 + w * unit, unit)]
                        done[to, unit_rows(2 * colour + w, p, q + (side - 1, 1)[j])] = v
                        if w == j:
                            sbuf[two[j], sent, pl.ds(AY2, unit)] = v

        c6, when = stage(6)

        @when
        def _():
            to = c6 % OUT_SLOTS
            for colour, one, two, p, q in colours:
                for j in range(2):
                    done[to, unit_rows(2 * colour + j, p, q + 2)] = rbuf[two[j], got, pl.ds(AY2, unit)]

            kind = (k - 6 * LAT) % 3

            @pl.when(c6 < first)
            def _():
                if kind:
                    take_quarters(kind - 1, c6, later_q)
                else:
                    for colour, one, two, p, q in colours:
                        for w in range(2):
                            v = done[to, quarter_rows(2 * colour + w, p)]
                            for j in range(2):
                                sbuf[one[j], sent, pl.ds(AX1 + w * quarter, quarter)] = v

            pl.when(c6 >= first)(lambda: take_quarters(kind, c6, first_q))

        c7, when = stage(7, first)

        def spread():
            to = c7 % OUT_SLOTS
            for colour, one, two, p, q in colours:
                for j in range(2):
                    for w in range(2):
                        v = rbuf[one[j], got, pl.ds(AX1 + w * quarter, quarter)]
                        done[to, quarter_rows(2 * colour + w, p + (side - 1, 1)[j])] = v
                        if w == j:
                            sbuf[one[j], sent, pl.ds(AX2, quarter)] = v

        if (k - 7 * LAT) % 3 == 0:
            when(spread)

        c8, when = stage(8, first)

        def finish():
            to = c8 % OUT_SLOTS
            for colour, one, two, p, q in colours:
                for j in range(2):
                    done[to, quarter_rows(2 * colour + j, p + 2)] = rbuf[one[j], got, pl.ds(AX2, quarter)]
            take_whole(c8)

        if (k - 8 * LAT) % 3 == 0:
            when(finish)

        for which in parts_of(k):
            start, stop = sent_in[which]

            @pl.when((i >= start) & (i < stop))
            def _(which=which):
                for link in range(4):
                    message(link, which, i).start()

    def weights(number, slot):
        layer, cols = 1 - number // blocks, at_rows((number % blocks) * panel, panel)
        return (
            pltpu.make_async_copy(wg_ref.at[layer, :, cols], wgu.at[slot, :, pl.ds(0, panel)], wsem.at[0, slot]),
            pltpu.make_async_copy(wu_ref.at[layer, :, cols], wgu.at[slot, :, pl.ds(panel, panel)], wsem.at[1, slot]),
            pltpu.make_async_copy(wd_ref.at[layer, cols, :], wdb.at[slot], wsem.at[2, slot]),
        )

    def take_in(_t, _):
        rows = at_rows(_t * tile, tile)
        a = normed(a_v[rows, :])
        a_v[rows, :] = a
        at_v[:, rows] = a.T
        return _

    def columns_of(number):
        return at_rows((number % 2) * 2 * panel, 2 * panel)

    def fetch(number):
        return pltpu.make_async_copy(kept_ref.at[number - blocks], acc.at[:, columns_of(number)], sem.at[number % 2])

    for c in weights(0, 0):
        c.start()
    gets = (pltpu.make_async_copy(h_ref, a_v, sem.at[0]), pltpu.make_async_copy(dy_ref, ct_v, sem.at[1]))
    for c in gets:
        c.start()
    for c in gets:
        c.wait()
    lax.fori_loop(0, tokens // tile, take_in, 0)

    def next_layer():
        get = pltpu.make_async_copy(h_ref, a_v, sem.at[0])
        get.start()
        get.wait()
        small = tile // 4

        def back(t, _):
            rows = at_rows(t * small, small)
            wide = a_v[rows, :].astype(F32)
            scale = scale_of(wide)
            by_a = acc[rows, :].astype(BF16).astype(F32)
            inner = jnp.mean(by_a * wide, -1, keepdims=True)
            by_h = by_a * scale - wide * (scale * scale * scale * inner)
            ct_v[rows, :] = ct_v[rows, :] + by_h.astype(BF16)
            return _

        lax.fori_loop(0, tokens // small, back, 0)
        get = pltpu.make_async_copy(x_ref, a_v, sem.at[0])
        get.start()
        get.wait()
        fetch(blocks).start()
        lax.fori_loop(0, tokens // tile, take_in, 0)

    def block(number, carry):
        slot = number % 2
        later = number < blocks
        i = 3 * number

        pl.when(number == blocks)(next_layer)

        for c in weights(number, slot):
            c.wait()

        @pl.when(number + 1 < 2 * blocks)
        def _():
            for c in weights(number + 1, 1 - slot):
                c.start()

        @pl.when(number >= blocks)
        def _():
            pltpu.make_async_copy(kept_ref.at[0], acc.at[:, columns_of(number)], sem.at[slot]).wait()

            @pl.when(number + 1 < 2 * blocks)
            def _():
                fetch(number + 1).start()

        def hidden(t, gu):
            rows = pl.ds(t * tile, tile)
            by_hidden = dot_t(ct_v[rows, :], wdb[slot]).astype(BF16).astype(F32)
            gate, up = gu[:, :panel], gu[:, panel:]
            sigmoid = jax.nn.sigmoid(gate)
            silu = gate * sigmoid
            hidt[:, rows] = (silu * up).astype(BF16).T
            dgu[rows, pl.ds(0, panel)] = (by_hidden * up * (sigmoid + silu * (1.0 - sigmoid))).astype(BF16)
            dgu[rows, pl.ds(panel, panel)] = (by_hidden * silu).astype(BF16)

        def hidden_half(part):
            tiles = tokens // tile // 2

            @pl.when(later)
            def _():
                for t in range(part * tiles, part * tiles + tiles):
                    hidden(t, dot(a_v[pl.ds(t * tile, tile), :], wgu[slot]))

            @pl.when(number >= blocks)
            def _():
                for t in range(part * tiles, part * tiles + tiles):
                    hidden(t, acc[pl.ds(t * tile, tile), columns_of(number)])

        hidden_half(0)

        @pl.when(number > 0)
        def _():
            tick(i - 1, 2)

        hidden_half(1)
        for k in range(PANELS):
            own[i % G_SLOTS, pl.ds(k * panel, panel)] = dot(hidt[...], ct_v[:, pl.ds(k * panel, panel)]).astype(BF16)
        tick(i, 0)
        for k in range(PANELS):
            v = dot(at_v[pl.ds(k * panel, panel), :], dgu[...]).astype(BF16)
            own[(i + 1) % G_SLOTS, pl.ds(k * panel, panel)] = v[:, :panel]
            own[(i + 2) % G_SLOTS, pl.ds(k * panel, panel)] = v[:, panel:]
        tick(i + 1, 1)

        @pl.when(later)
        def _():
            for t in range(tokens // tile):
                rows = pl.ds(t * tile, tile)
                v = dot_t(dgu[rows, :], wgu[slot])
                acc[rows, :] = jnp.where(number == 0, v, acc[rows, :] + v)

        return carry

    lax.fori_loop(0, 2 * blocks, block, 0)

    tick(chunks - 1, 2)

    def drain(t, _):
        for k in range(3):
            tick(chunks + 3 * t + k, k)
        return _

    lax.fori_loop(0, (6 * LAT + 2) // 3, drain, 0)
    for c in range(chunks - OUT_SLOTS, chunks):
        (wait_whole if c < first and c % 3 == 0 else wait_quarters)(c)


def backward(side, x, h, kept, dy, wg, wu, wd):
    tokens, d = x.shape
    panel = d // PANELS
    blocks = wg.shape[2] // panel
    rows = 6 * (panel // side + panel // side // side)
    hbm = pl.BlockSpec(memory_space=pl.ANY)
    return pl.pallas_call(
        functools.partial(backward_kernel, side),
        out_shape=(jax.ShapeDtypeStruct((blocks, d, panel), BF16),)
        + tuple(jax.ShapeDtypeStruct((2, n, blocks, panel // side, panel), BF16) for n in (2, 3) for _ in range(2)),
        in_specs=[hbm] * 7,
        out_specs=(hbm,) * 5,
        scratch_shapes=[
            pltpu.VMEM((tokens, d), BF16),
            pltpu.VMEM((d, tokens), BF16),
            pltpu.VMEM((tokens, d), BF16),
            pltpu.VMEM((tokens, d), F32),
            pltpu.VMEM((2, d, 2 * panel), BF16),
            pltpu.VMEM((2, panel, d), BF16),
            pltpu.VMEM((panel, tokens), BF16),
            pltpu.VMEM((tokens, 2 * panel), BF16),
            pltpu.VMEM((G_SLOTS, d, panel), BF16),
            pltpu.VMEM((G_SLOTS, 2, 2 * panel // side, panel), F32),
            pltpu.VMEM((OUT_SLOTS, d, panel), BF16),
            pltpu.VMEM((4, LAT, rows, panel), BF16),
            pltpu.VMEM((4, 2 * LAT, rows, panel), BF16),
            pltpu.SemaphoreType.DMA((2,)),
            pltpu.SemaphoreType.DMA((3, 2)),
            pltpu.SemaphoreType.DMA((OUT_SLOTS,)),
            pltpu.SemaphoreType.DMA((4, 4, LAT)),
            pltpu.SemaphoreType.DMA((4, 4, 2 * LAT)),
        ],
        compiler_params=pltpu.CompilerParams(collective_id=0, has_side_effects=True, vmem_limit_bytes=VMEM_LIMIT),
        cost_estimate=pl.CostEstimate(flops=24 * tokens * d * wg.shape[2], bytes_accessed=4 * 3 * wg.size, transcendentals=2 * tokens * wg.shape[2]),
        name="backward",
    )(x, h, kept, dy, wg, wu, wd)


def adamw(w, m, v, g):
    m = 0.9 * m + 0.1 * g
    v = 0.95 * v + 0.05 * g * g
    step = m * lax.rsqrt(v + 1e-8) + 0.1 * w
    return (w - 0.02 * step).astype(BF16), m, v


RING = 4
AHEAD = 2


def update_kernel(side, plan, sources, fresh, *refs):
    wmv, refs = (refs[0:3], refs[3:6], refs[6:9]), refs[9:]
    source, refs = refs[:sources], refs[sources:]
    refs = refs if fresh else refs[9:]
    new, refs = (refs[0:3], refs[3:6], refs[6:9]), refs[9:]
    tall, flat, gbuf, isem, osem = refs[0:3], refs[3:6], refs[6], refs[7], refs[8]
    _, quarter, panel = gbuf.shape[2:]
    me = lax.axis_index("dp")
    position = (me // side, me % side)
    units = plan

    def arrays(refs, u):
        layer, kind, start, blocks, colour, k, relative, _ = units[u]
        k = (position[colour] + k + side) % side if relative else k
        if kind == 0:
            at = (layer, pl.ds(start, blocks), k, slice(None), pl.ds(2 * colour * panel, 2 * panel))
        else:
            at = (layer, pl.ds(2 * colour, 2), k, slice(None), pl.ds(start * panel, blocks * panel))
        return [r[(2, 0, 1)[kind]].at[at] for r in refs]

    def buffers(u):
        blocks = units[u][3]
        if units[u][1] == 0:
            return [b.at[u % RING, pl.ds(0, blocks)] for b in flat]
        return [b.at[u % RING, :, :, pl.ds(0, blocks * panel)] for b in tall]

    def copies_in(u):
        _, _, start, blocks, _, _, _, halves = units[u]
        slot = u % RING
        cs = [pltpu.make_async_copy(a, b, isem.at[n, slot]) for n, (a, b) in enumerate(zip(arrays(wmv, u), buffers(u)))]
        for j, (which, index, rows) in enumerate(halves):
            ref = source[which] if index is None else source[which].at[index]
            ref = ref.at[pl.ds(start, blocks), pl.ds(rows, quarter)]
            cs.append(pltpu.make_async_copy(ref, gbuf.at[slot, j, pl.ds(0, blocks)], isem.at[3 + j, slot]))
        return cs

    def copies_out(u):
        return [pltpu.make_async_copy(b, a, osem.at[n, u % RING]) for n, (a, b) in enumerate(zip(arrays(new, u), buffers(u)))]

    def begin(u):
        for c in copies_in(u):
            c.start()

    for u in range(min(AHEAD, len(units))):
        begin(u)
    for u in range(len(units)):
        if u + AHEAD < len(units):
            if u + AHEAD >= RING:
                for c in copies_out(u + AHEAD - RING):
                    c.wait()
            begin(u + AHEAD)
        for c in copies_in(u):
            c.wait()
        slot = u % RING
        w_b, m_b, v_b = flat if units[u][1] == 0 else tall

        def part(b, carry):
            for j in range(2):
                if units[u][1] == 0:
                    at = (slot, b, slice(None), pl.ds(j * panel, panel))
                else:
                    at = (slot, j, slice(None), at_rows(b * panel, panel))
                w_b[at], m_b[at], v_b[at] = adamw(w_b[at].astype(F32), m_b[at], v_b[at], gbuf[slot, j, b].astype(F32))
            return carry

        lax.fori_loop(0, units[u][3], part, 0)
        for c in copies_out(u):
            c.start()
    for u in range(max(0, len(units) - RING), len(units)):
        for c in copies_out(u):
            c.wait()


def update(side, plan, wmv, sources, old):
    _, _, _, quarter, ff = wmv[0].shape
    blocks = max(one[3] for one in plan)
    panel = ff // wmv[2].shape[1]
    hbm = pl.BlockSpec(memory_space=pl.ANY)
    size = sum(one[3] for one in plan) * 2 * quarter * panel
    return pl.pallas_call(
        functools.partial(update_kernel, side, plan, len(sources), old is None),
        out_shape=tuple(jax.ShapeDtypeStruct(a.shape, a.dtype) for a in wmv),
        in_specs=[hbm] * (9 + len(sources) + (0 if old is None else 9)),
        out_specs=(hbm,) * 9,
        input_output_aliases={} if old is None else {9 + len(sources) + n: n for n in range(9)},
        scratch_shapes=[pltpu.VMEM((RING, 2, quarter, blocks * panel), t) for t in (BF16, F32, F32)]
        + [pltpu.VMEM((RING, blocks, quarter, 2 * panel), t) for t in (BF16, F32, F32)]
        + [pltpu.VMEM((RING, 2, blocks, quarter, panel), BF16), pltpu.SemaphoreType.DMA((5, RING)), pltpu.SemaphoreType.DMA((3, RING))],
        compiler_params=pltpu.CompilerParams(vmem_limit_bytes=VMEM_LIMIT),
        cost_estimate=pl.CostEstimate(flops=size * 6000, bytes_accessed=22 * size, transcendentals=size),
        name="update",
    )(*wmv, *sources, *(old or ()))


def solution(mesh):
    side = math.isqrt(mesh.shape["dp"])
    spots = [(x, y) for x in range(side) for y in range(side)]

    def shift(dx, dy):
        return [(x * side + y, (x + dx) % side * side + (y + dy) % side) for x, y in spots]

    ways = ((shift(1, 0), shift(-1, 0)), (shift(0, 1), shift(0, -1)))

    def step(x, dy, *arrays):
        weights = arrays[:3]
        x, dy = x[0], dy[0]
        d, ff = weights[0].shape[1:]
        panel = d // PANELS
        quarter, blocks = panel // side, ff // panel
        h, kept = forward(x, *weights)
        whole, *quarters = backward(side, x, h, kept, dy, *weights)
        wmv = [a.reshape(a.shape[0], blocks, side, quarter, d) if n % 3 == 2 else a.reshape(a.shape[0], PANELS, side, quarter, ff) for n, a in enumerate(arrays)]

        def near(quarters):
            return [[lax.ppermute(q, "dp", ways[c][way]) for c, q in enumerate(quarters)] for way in range(2)]

        def far(near, way):
            return [lax.ppermute(q, "dp", ways[c][way]) for c, q in enumerate(near[way])]

        def pieces(layer, kinds, colour, k, relative, halves):
            return [(layer, kind, 0, blocks, colour, k, relative, halves(kind)) for kind in kinds]

        def join(parts):
            return [one for part in parts for one in part]

        def three(layer, kinds):
            return join(
                pieces(layer, kinds, c, r, True, lambda kind: [(2 * s + c, (j, kind - kinds[0]), 0) for j in range(2)])
                for c in range(2)
                for s, r in enumerate((0, -1, 1))
            )

        def last(layer, kinds, at):
            return join(pieces(layer, kinds, c, 2, True, lambda kind: [(at + c, (j, kind - kinds[0]), 0) for j in range(2)]) for c in range(2))

        def known(layer, kind):
            return join(
                pieces(layer, (kind,), c, k, False, lambda _: [(0, None, (2 * c + j) * panel + k * quarter) for j in range(2)])
                for c in range(2)
                for k in range(side)
            )

        later, first = quarters[:2], quarters[2:]
        later_near, first_near = near(later), near(first)
        new = update(side, known(1, 0), wmv, [whole], None)
        later_far = far(later_near, 0)
        new = update(side, three(1, (1, 2)), wmv, join([later, *later_near]), new)
        first_far = far(first_near, 1)
        new = update(side, three(0, (0, 1, 2)), wmv, join([first, *first_near]), new)
        new = update(side, last(1, (1, 2), 0) + last(0, (0, 1, 2), 2), wmv, [*later_far, *first_far], new)
        return tuple(a.reshape(b.shape) for a, b in zip(new, arrays, strict=True))

    return jax.shard_map(
        step,
        mesh=mesh,
        in_specs=(P(("rep", "dp"), None, None),) * 2 + (P(None, None, None),) * 9,
        out_specs=(P("rep", None, None),) * 9,
        check_vma=False,
    )
```

```python
import functools
import math

import jax
import jax.numpy as jnp
from jax import lax
from jax.experimental import pallas as pl
from jax.experimental.pallas import tpu as pltpu
from jax.sharding import PartitionSpec as P

MESH = pl.DeviceIdType.MESH
F32, BF16 = jnp.float32, jnp.bfloat16
PANELS = 4
LAT = 2
STAGES = 8
G_SLOTS = 2 * LAT + 2
OUT_SLOTS = 4 * LAT + 3
VMEM_LIMIT = 62 * 2**20


def dot(a, b):
    return jnp.dot(a, b, preferred_element_type=F32)


def dot_t(a, b):
    return lax.dot_general(a, b, (((1,), (1,)), ((), ())), preferred_element_type=F32)


def scale_of(wide):
    return lax.rsqrt(jnp.mean(wide**2, -1, keepdims=True) + 1e-6)


def normed(h):
    wide = h.astype(F32)
    return (wide * scale_of(wide)).astype(BF16)


def at_rows(start, size):
    return pl.ds(pl.multiple_of(start, size), size)


def layers_kernel(side, x_ref, dy_ref, wg_ref, wu_ref, wd_ref, g_ref, *refs):
    later_q, first_q, kept_ref, refs = refs[0:2], refs[2:4], refs[4], refs[5:]
    a_v, at_v, ct_v, acc, wgu, wdb, hidt, dgu, own, part1, done, sbuf, rbuf, x_v, gu_v, sem, wsem, osem, ssem, rsem, ksem = refs
    tokens, d = a_v.shape
    panel = wdb.shape[1]
    blocks = wg_ref.shape[2] // panel
    quarter, unit = panel // side, panel // side // side
    tile = min(512, tokens // 4)
    first, chunks = blocks * 3, 2 * blocks * 3
    half = 3 * quarter + 3 * unit
    X1, X2, Y1, Y2 = 0, quarter, 3 * quarter, 3 * quarter + unit
    AY1, AY2, AX1, AX2 = half, half + 2 * unit, half + 3 * unit, half + 3 * unit + 2 * quarter

    rep, me = lax.axis_index("rep"), lax.axis_index("dp")
    px, py = me // side, me % side
    device = lambda x, y: (rep, (x % side) * side + y % side)
    near = (device(px + 1, py), device(px + side - 1, py), device(px, py + 1), device(px, py + side - 1))
    colours = ((0, (0, 1), (2, 3), px, py), (1, (2, 3), (0, 1), py, px))

    barrier = pltpu.get_barrier_semaphore()
    for n in near:
        pl.semaphore_signal(barrier, inc=1, device_id=n, device_id_type=MESH)

    parts = ((X1, Y1), (Y1, AX1), (AX1, AX2), (AX2, 2 * half))
    sent_in = ((0, chunks + LAT), (2 * LAT, chunks + 5 * LAT), (6 * LAT, first + 6 * LAT), (7 * LAT, first + 7 * LAT))

    def parts_of(k):
        return [which for which in range(4) if which < 2 or (k - (which + 4) * LAT) % 3 == 0]


    def message(link, which, i):
        rows = pl.ds(parts[which][0], parts[which][1] - parts[which][0])
        return pltpu.make_async_remote_copy(
            src_ref=sbuf.at[link, i % LAT, rows],
            dst_ref=rbuf.at[link, i % (2 * LAT), rows],
            send_sem=ssem.at[which, link, i % LAT],
            recv_sem=rsem.at[which, link, i % (2 * LAT)],
            device_id=near[link],
            device_id_type=MESH,
        )

    def take_whole(c):
        pltpu.make_async_copy(done.at[c % OUT_SLOTS], g_ref.at[c // 3], osem.at[c % OUT_SLOTS]).start()

    def take_quarters(k, c, refs):
        slot = c % OUT_SLOTS
        for colour, _, _, p, _ in colours:
            for j in range(2):
                rows = at_rows((2 * colour + j) * panel + p * quarter, quarter)
                to = refs[colour].at[j, k, (c // 3) % blocks]
                pltpu.make_async_copy(done.at[slot, rows], to, osem.at[slot]).start()

    def wait_whole(c):
        pltpu.make_async_copy(done.at[c % OUT_SLOTS], g_ref.at[0], osem.at[c % OUT_SLOTS]).wait()

    def wait_quarters(c):
        rows = pl.ds(0, quarter)
        for _ in range(PANELS):
            pltpu.make_async_copy(done.at[c % OUT_SLOTS, rows], first_q[0].at[0, 0, 0], osem.at[c % OUT_SLOTS]).wait()

    def tick(i, k):
        sent, got = i % LAT, (i + LAT) % (2 * LAT)

        for which in parts_of((k - LAT) % 3):
            start, stop = sent_in[which]

            @pl.when((i >= start + LAT) & (i < stop + LAT))
            def _(which=which):
                for link in range(4):
                    message(link, which, i + LAT).wait_send()
                    message(link, which, i + LAT).wait_recv()

        def stage(s, stop=chunks):
            c = i - s * LAT
            return c, pl.when((c >= 0) & (c < stop))

        def quarter_rows(p, k):
            return at_rows(p * panel + (k % side) * quarter, quarter)

        def unit_rows(p, k, j):
            return at_rows(p * panel + (k % side) * quarter + (j % side) * unit, unit)

        def unit_of(p, j):
            return at_rows(p * quarter + (j % side) * unit, unit)

        wide = lambda v: v.astype(F32)

        c0, when = stage(0)

        @when
        def _():
            for colour, one, two, p, q in colours:
                for j in range(2):
                    sbuf[one[j], sent, pl.ds(X1, quarter)] = own[c0 % G_SLOTS, quarter_rows(2 * colour + j, p + 2)]

        c1, when = stage(1)

        @when
        def _():
            slot = c1 % G_SLOTS
            for colour, one, two, p, q in colours:
                for j in range(2):
                    to = p + (1, side - 1)[j]
                    for w in range(2):
                        v = own[slot, quarter_rows(2 * colour + w, to)]
                        if w == j:
                            v = (wide(v) + wide(rbuf[one[j], got, pl.ds(X1, quarter)])).astype(BF16)
                        sbuf[one[j], sent, pl.ds(X2 + w * quarter, quarter)] = v

        c2, when = stage(2)

        @when
        def _():
            slot = c2 % G_SLOTS
            for colour, one, two, p, q in colours:
                for w in range(2):
                    rows = pl.ds(X2 + w * quarter, quarter)
                    part1[slot, colour, pl.ds(w * quarter, quarter)] = (
                        wide(own[slot, quarter_rows(2 * colour + w, p)]) + wide(rbuf[one[0], got, rows]) + wide(rbuf[one[1], got, rows])
                    )
                for j in range(2):
                    sbuf[two[j], sent, pl.ds(Y1, unit)] = part1[slot, colour, unit_of(j, q + 2)].astype(BF16)

        c3, when = stage(3)

        @when
        def _():
            slot = c3 % G_SLOTS
            for colour, one, two, p, q in colours:
                for j in range(2):
                    to = q + (1, side - 1)[j]
                    for w in range(2):
                        v = part1[slot, colour, unit_of(w, to)]
                        if w == j:
                            v = v + wide(rbuf[two[j], got, pl.ds(Y1, unit)])
                        sbuf[two[j], sent, pl.ds(Y2 + w * unit, unit)] = v.astype(BF16)

        c4, when = stage(4)

        @when
        def _():
            if (k - 4 * LAT - OUT_SLOTS) % 3 == 0:

                @pl.when((c4 >= OUT_SLOTS) & (c4 < first + OUT_SLOTS))
                def _():
                    wait_whole(c4)

                pl.when(c4 >= first + OUT_SLOTS)(lambda: wait_quarters(c4))
            else:
                pl.when(c4 >= OUT_SLOTS)(lambda: wait_quarters(c4))

            slot, to = c4 % G_SLOTS, c4 % OUT_SLOTS
            for colour, one, two, p, q in colours:
                for w in range(2):
                    rows = pl.ds(Y2 + w * unit, unit)
                    v = part1[slot, colour, unit_of(w, q)] + wide(rbuf[two[0], got, rows]) + wide(rbuf[two[1], got, rows])
                    v = v.astype(BF16)
                    done[to, unit_rows(2 * colour + w, p, q)] = v
                    for j in range(2):
                        sbuf[two[j], sent, pl.ds(AY1 + w * unit, unit)] = v

        c5, when = stage(5)

        @when
        def _():
            to = c5 % OUT_SLOTS
            for colour, one, two, p, q in colours:
                for j in range(2):
                    for w in range(2):
                        v = rbuf[two[j], got, pl.ds(AY1 + w * unit, unit)]
                        done[to, unit_rows(2 * colour + w, p, q + (side - 1, 1)[j])] = v
                        if w == j:
                            sbuf[two[j], sent, pl.ds(AY2, unit)] = v

        c6, when = stage(6)

        @when
        def _():
            to = c6 % OUT_SLOTS
            for colour, one, two, p, q in colours:
                for j in range(2):
                    done[to, unit_rows(2 * colour + j, p, q + 2)] = rbuf[two[j], got, pl.ds(AY2, unit)]

            kind = (k - 6 * LAT) % 3

            @pl.when(c6 < first)
            def _():
                if kind:
                    take_quarters(kind - 1, c6, later_q)
                else:
                    for colour, one, two, p, q in colours:
                        for w in range(2):
                            v = done[to, quarter_rows(2 * colour + w, p)]
                            for j in range(2):
                                sbuf[one[j], sent, pl.ds(AX1 + w * quarter, quarter)] = v

            pl.when(c6 >= first)(lambda: take_quarters(kind, c6, first_q))

        c7, when = stage(7, first)

        def spread():
            to = c7 % OUT_SLOTS
            for colour, one, two, p, q in colours:
                for j in range(2):
                    for w in range(2):
                        v = rbuf[one[j], got, pl.ds(AX1 + w * quarter, quarter)]
                        done[to, quarter_rows(2 * colour + w, p + (side - 1, 1)[j])] = v
                        if w == j:
                            sbuf[one[j], sent, pl.ds(AX2, quarter)] = v

        if (k - 7 * LAT) % 3 == 0:
            when(spread)

        c8, when = stage(8, first)

        def finish():
            to = c8 % OUT_SLOTS
            for colour, one, two, p, q in colours:
                for j in range(2):
                    done[to, quarter_rows(2 * colour + j, p + 2)] = rbuf[one[j], got, pl.ds(AX2, quarter)]
            take_whole(c8)

        if (k - 8 * LAT) % 3 == 0:
            when(finish)

        for which in parts_of(k):
            start, stop = sent_in[which]

            @pl.when((i >= start) & (i < stop))
            def _(which=which):
                for link in range(4):
                    message(link, which, i).start()

    def weights(turn):
        slot, layer, cols = turn % 2, (turn // blocks) % 2, at_rows((turn % blocks) * panel, panel)
        return (
            pltpu.make_async_copy(wg_ref.at[layer, :, cols], wgu.at[slot, :, pl.ds(0, panel)], wsem.at[0, slot]),
            pltpu.make_async_copy(wu_ref.at[layer, :, cols], wgu.at[slot, :, pl.ds(panel, panel)], wsem.at[1, slot]),
            pltpu.make_async_copy(wd_ref.at[layer, cols, :], wdb.at[slot], wsem.at[2, slot]),
        )

    def take_in(_t, _):
        rows = at_rows(_t * tile, tile)
        a = normed(a_v[rows, :])
        a_v[rows, :] = a
        at_v[:, rows] = a.T
        return _

    def columns_of(number):
        return at_rows((number % 2) * 2 * panel, 2 * panel)

    def fetch(number):
        return pltpu.make_async_copy(kept_ref.at[number - blocks], acc.at[:, columns_of(number)], sem.at[number % 2])

    def keep(b):
        return pltpu.make_async_copy(gu_v.at[b % 2], kept_ref.at[b], ksem.at[b % 2])

    gets = (pltpu.make_async_copy(x_ref, x_v, sem.at[0]), pltpu.make_async_copy(dy_ref, ct_v, sem.at[1]))
    gets[0].start()
    for c in weights(0):
        c.start()
    gets[0].wait()
    gets[1].start()

    def first_norm(t, _):
        rows = at_rows(t * tile, tile)
        a_v[rows, :] = normed(x_v[rows, :])
        acc[rows, :] = jnp.zeros((tile, d), F32)
        return _

    lax.fori_loop(0, tokens // tile, first_norm, 0)

    def forward(b, carry):
        slot = b % 2
        for c in weights(b):
            c.wait()
        for c in weights(b + 1):
            c.start()

        @pl.when(b >= 2)
        def _():
            keep(b).wait()

        for t in range(tokens // tile):
            rows = pl.ds(t * tile, tile)
            gu = dot(a_v[rows, :], wgu[slot])
            gu_v[slot, rows, :] = gu
            hidden = (jax.nn.silu(gu[:, :panel]) * gu[:, panel:]).astype(BF16)
            acc[rows, :] += dot(hidden, wdb[slot])
        keep(b).start()
        return carry

    lax.fori_loop(0, blocks, forward, 0)

    def between(t, _):
        rows = at_rows(t * tile, tile)
        x_v[rows, :] = x_v[rows, :] + acc[rows, :].astype(BF16)
        a = normed(x_v[rows, :])
        a_v[rows, :] = a
        at_v[:, rows] = a.T
        return _

    lax.fori_loop(0, tokens // tile, between, 0)
    for b in range(max(0, blocks - 2), blocks):
        keep(b).wait()
    gets[1].wait()
    pl.semaphore_wait(barrier, 4)

    def next_layer():
        get = pltpu.make_async_copy(x_ref, a_v, sem.at[0])
        get.start()
        small = tile // 4

        def back(t, _):
            rows = at_rows(t * small, small)
            wide = x_v[rows, :].astype(F32)
            scale = scale_of(wide)
            by_a = acc[rows, :].astype(BF16).astype(F32)
            inner = jnp.mean(by_a * wide, -1, keepdims=True)
            by_h = by_a * scale - wide * (scale * scale * scale * inner)
            ct_v[rows, :] = ct_v[rows, :] + by_h.astype(BF16)
            return _

        lax.fori_loop(0, tokens // small, back, 0)
        get.wait()
        fetch(blocks).start()
        lax.fori_loop(0, tokens // tile, take_in, 0)

    def block(number, carry):
        turn = blocks + number
        slot = turn % 2
        later = number < blocks
        i = 3 * number

        pl.when(number == blocks)(next_layer)

        for c in weights(turn):
            c.wait()

        @pl.when(number + 1 < 2 * blocks)
        def _():
            for c in weights(turn + 1):
                c.start()

        @pl.when(number >= blocks)
        def _():
            pltpu.make_async_copy(kept_ref.at[0], acc.at[:, columns_of(number)], sem.at[number % 2]).wait()

            @pl.when(number + 1 < 2 * blocks)
            def _():
                fetch(number + 1).start()

        def hidden(t, gu):
            rows = pl.ds(t * tile, tile)
            by_hidden = dot_t(ct_v[rows, :], wdb[slot]).astype(BF16).astype(F32)
            gate, up = gu[:, :panel], gu[:, panel:]
            sigmoid = jax.nn.sigmoid(gate)
            silu = gate * sigmoid
            hidt[:, rows] = (silu * up).astype(BF16).T
            dgu[rows, pl.ds(0, panel)] = (by_hidden * up * (sigmoid + silu * (1.0 - sigmoid))).astype(BF16)
            dgu[rows, pl.ds(panel, panel)] = (by_hidden * silu).astype(BF16)

        def hidden_half(part):
            tiles = tokens // tile // 2

            @pl.when(later)
            def _():
                for t in range(part * tiles, part * tiles + tiles):
                    hidden(t, dot(a_v[pl.ds(t * tile, tile), :], wgu[slot]))

            @pl.when(number >= blocks)
            def _():
                for t in range(part * tiles, part * tiles + tiles):
                    hidden(t, acc[pl.ds(t * tile, tile), columns_of(number)])

        hidden_half(0)

        @pl.when(number > 0)
        def _():
            tick(i - 1, 2)

        hidden_half(1)
        for k in range(PANELS):
            own[i % G_SLOTS, pl.ds(k * panel, panel)] = dot(hidt[...], ct_v[:, pl.ds(k * panel, panel)]).astype(BF16)
        tick(i, 0)
        for k in range(PANELS):
            v = dot(at_v[pl.ds(k * panel, panel), :], dgu[...]).astype(BF16)
            own[(i + 1) % G_SLOTS, pl.ds(k * panel, panel)] = v[:, :panel]
            own[(i + 2) % G_SLOTS, pl.ds(k * panel, panel)] = v[:, panel:]
        tick(i + 1, 1)

        @pl.when(later)
        def _():
            for t in range(tokens // tile):
                rows = pl.ds(t * tile, tile)
                v = dot_t(dgu[rows, :], wgu[slot])
                acc[rows, :] = jnp.where(number == 0, v, acc[rows, :] + v)

        return carry

    lax.fori_loop(0, 2 * blocks, block, 0)

    tick(chunks - 1, 2)

    def drain(t, _):
        for k in range(3):
            tick(chunks + 3 * t + k, k)
        return _

    lax.fori_loop(0, (6 * LAT + 2) // 3, drain, 0)
    for c in range(chunks - OUT_SLOTS, chunks):
        (wait_whole if c < first and c % 3 == 0 else wait_quarters)(c)


def run_layers(side, x, dy, wg, wu, wd):
    tokens, d = x.shape
    panel = d // PANELS
    blocks = wg.shape[2] // panel
    rows = 6 * (panel // side + panel // side // side)
    hbm = pl.BlockSpec(memory_space=pl.ANY)
    return pl.pallas_call(
        functools.partial(layers_kernel, side),
        out_shape=(jax.ShapeDtypeStruct((blocks, d, panel), BF16),)
        + tuple(jax.ShapeDtypeStruct((2, n, blocks, panel // side, panel), BF16) for n in (2, 3) for _ in range(2))
        + (jax.ShapeDtypeStruct((blocks, tokens, 2 * panel), F32),),
        in_specs=[hbm] * 5,
        out_specs=(hbm,) * 6,
        scratch_shapes=[
            pltpu.VMEM((tokens, d), BF16),
            pltpu.VMEM((d, tokens), BF16),
            pltpu.VMEM((tokens, d), BF16),
            pltpu.VMEM((tokens, d), F32),
            pltpu.VMEM((2, d, 2 * panel), BF16),
            pltpu.VMEM((2, panel, d), BF16),
            pltpu.VMEM((panel, tokens), BF16),
            pltpu.VMEM((tokens, 2 * panel), BF16),
            pltpu.VMEM((G_SLOTS, d, panel), BF16),
            pltpu.VMEM((G_SLOTS, 2, 2 * panel // side, panel), F32),
            pltpu.VMEM((OUT_SLOTS, d, panel), BF16),
            pltpu.VMEM((4, LAT, rows, panel), BF16),
            pltpu.VMEM((4, 2 * LAT, rows, panel), BF16),
            pltpu.VMEM((tokens, d), BF16),
            pltpu.VMEM((2, tokens, 2 * panel), F32),
            pltpu.SemaphoreType.DMA((2,)),
            pltpu.SemaphoreType.DMA((3, 2)),
            pltpu.SemaphoreType.DMA((OUT_SLOTS,)),
            pltpu.SemaphoreType.DMA((4, 4, LAT)),
            pltpu.SemaphoreType.DMA((4, 4, 2 * LAT)),
            pltpu.SemaphoreType.DMA((2,)),
        ],
        compiler_params=pltpu.CompilerParams(collective_id=0, has_side_effects=True, vmem_limit_bytes=VMEM_LIMIT),
        cost_estimate=pl.CostEstimate(flops=30 * tokens * d * wg.shape[2], bytes_accessed=4 * 3 * wg.size, transcendentals=2 * tokens * wg.shape[2]),
        name="layers",
    )(x, dy, wg, wu, wd)


def adamw(w, m, v, g):
    m = 0.9 * m + 0.1 * g
    v = 0.95 * v + 0.05 * g * g
    step = m * lax.rsqrt(v + 1e-8) + 0.1 * w
    return (w - 0.02 * step).astype(BF16), m, v


RING = 4
AHEAD = 2


def update_kernel(side, plan, sources, fresh, *refs):
    wmv, refs = (refs[0:3], refs[3:6], refs[6:9]), refs[9:]
    source, refs = refs[:sources], refs[sources:]
    refs = refs if fresh else refs[9:]
    new, refs = (refs[0:3], refs[3:6], refs[6:9]), refs[9:]
    tall, flat, gbuf, isem, osem = refs[0:3], refs[3:6], refs[6], refs[7], refs[8]
    _, quarter, panel = gbuf.shape[2:]
    me = lax.axis_index("dp")
    position = (me // side, me % side)
    units = plan

    def arrays(refs, u):
        layer, kind, start, blocks, colour, k, relative, _ = units[u]
        k = (position[colour] + k + side) % side if relative else k
        if kind == 0:
            at = (layer, pl.ds(start, blocks), k, slice(None), pl.ds(2 * colour * panel, 2 * panel))
        else:
            at = (layer, pl.ds(2 * colour, 2), k, slice(None), pl.ds(start * panel, blocks * panel))
        return [r[(2, 0, 1)[kind]].at[at] for r in refs]

    def buffers(u):
        blocks = units[u][3]
        if units[u][1] == 0:
            return [b.at[u % RING, pl.ds(0, blocks)] for b in flat]
        return [b.at[u % RING, :, :, pl.ds(0, blocks * panel)] for b in tall]

    def copies_in(u):
        _, _, start, blocks, _, _, _, halves = units[u]
        slot = u % RING
        cs = [pltpu.make_async_copy(a, b, isem.at[n, slot]) for n, (a, b) in enumerate(zip(arrays(wmv, u), buffers(u)))]
        for j, (which, index, rows) in enumerate(halves):
            ref = source[which] if index is None else source[which].at[index]
            ref = ref.at[pl.ds(start, blocks), pl.ds(rows, quarter)]
            cs.append(pltpu.make_async_copy(ref, gbuf.at[slot, j, pl.ds(0, blocks)], isem.at[3 + j, slot]))
        return cs

    def copies_out(u):
        return [pltpu.make_async_copy(b, a, osem.at[n, u % RING]) for n, (a, b) in enumerate(zip(arrays(new, u), buffers(u)))]

    def begin(u):
        for c in copies_in(u):
            c.start()

    for u in range(min(AHEAD, len(units))):
        begin(u)
    for u in range(len(units)):
        if u + AHEAD < len(units):
            if u + AHEAD >= RING:
                for c in copies_out(u + AHEAD - RING):
                    c.wait()
            begin(u + AHEAD)
        for c in copies_in(u):
            c.wait()
        slot = u % RING
        w_b, m_b, v_b = flat if units[u][1] == 0 else tall

        def part(b, carry):
            for j in range(2):
                if units[u][1] == 0:
                    at = (slot, b, slice(None), pl.ds(j * panel, panel))
                else:
                    at = (slot, j, slice(None), at_rows(b * panel, panel))
                w_b[at], m_b[at], v_b[at] = adamw(w_b[at].astype(F32), m_b[at], v_b[at], gbuf[slot, j, b].astype(F32))
            return carry

        lax.fori_loop(0, units[u][3], part, 0)
        for c in copies_out(u):
            c.start()
    for u in range(max(0, len(units) - RING), len(units)):
        for c in copies_out(u):
            c.wait()


def update(side, plan, wmv, sources, old):
    _, _, _, quarter, ff = wmv[0].shape
    blocks = max(one[3] for one in plan)
    panel = ff // wmv[2].shape[1]
    hbm = pl.BlockSpec(memory_space=pl.ANY)
    size = sum(one[3] for one in plan) * 2 * quarter * panel
    return pl.pallas_call(
        functools.partial(update_kernel, side, plan, len(sources), old is None),
        out_shape=tuple(jax.ShapeDtypeStruct(a.shape, a.dtype) for a in wmv),
        in_specs=[hbm] * (9 + len(sources) + (0 if old is None else 9)),
        out_specs=(hbm,) * 9,
        input_output_aliases={} if old is None else {9 + len(sources) + n: n for n in range(9)},
        scratch_shapes=[pltpu.VMEM((RING, 2, quarter, blocks * panel), t) for t in (BF16, F32, F32)]
        + [pltpu.VMEM((RING, blocks, quarter, 2 * panel), t) for t in (BF16, F32, F32)]
        + [pltpu.VMEM((RING, 2, blocks, quarter, panel), BF16), pltpu.SemaphoreType.DMA((5, RING)), pltpu.SemaphoreType.DMA((3, RING))],
        compiler_params=pltpu.CompilerParams(vmem_limit_bytes=VMEM_LIMIT),
        cost_estimate=pl.CostEstimate(flops=size * 6000, bytes_accessed=22 * size, transcendentals=size),
        name="update",
    )(*wmv, *sources, *(old or ()))


def solution(mesh):
    side = math.isqrt(mesh.shape["dp"])
    spots = [(x, y) for x in range(side) for y in range(side)]

    def shift(dx, dy):
        return [(x * side + y, (x + dx) % side * side + (y + dy) % side) for x, y in spots]

    ways = ((shift(1, 0), shift(-1, 0)), (shift(0, 1), shift(0, -1)))

    def step(x, dy, *arrays):
        weights = arrays[:3]
        x, dy = x[0], dy[0]
        d, ff = weights[0].shape[1:]
        panel = d // PANELS
        quarter, blocks = panel // side, ff // panel
        whole, *quarters, _ = run_layers(side, x, dy, *weights)
        wmv = [a.reshape(a.shape[0], blocks, side, quarter, d) if n % 3 == 2 else a.reshape(a.shape[0], PANELS, side, quarter, ff) for n, a in enumerate(arrays)]

        def near(quarters):
            return [[lax.ppermute(q, "dp", ways[c][way]) for c, q in enumerate(quarters)] for way in range(2)]

        def far(near, way):
            return [lax.ppermute(q, "dp", ways[c][way]) for c, q in enumerate(near[way])]

        def pieces(layer, kinds, colour, k, relative, halves):
            return [(layer, kind, 0, blocks, colour, k, relative, halves(kind)) for kind in kinds]

        def join(parts):
            return [one for part in parts for one in part]

        def three(layer, kinds):
            return join(
                pieces(layer, kinds, c, r, True, lambda kind: [(2 * s + c, (j, kind - kinds[0]), 0) for j in range(2)])
                for c in range(2)
                for s, r in enumerate((0, -1, 1))
            )

        def last(layer, kinds, at):
            return join(pieces(layer, kinds, c, 2, True, lambda kind: [(at + c, (j, kind - kinds[0]), 0) for j in range(2)]) for c in range(2))

        def known(layer, kind):
            return join(
                pieces(layer, (kind,), c, k, False, lambda _: [(0, None, (2 * c + j) * panel + k * quarter) for j in range(2)])
                for c in range(2)
                for k in range(side)
            )

        later, first = quarters[:2], quarters[2:]
        later_near, first_near = near(later), near(first)
        new = update(side, known(1, 0), wmv, [whole], None)
        later_far = far(later_near, 0)
        new = update(side, three(1, (1, 2)), wmv, join([later, *later_near]), new)
        first_far = far(first_near, 1)
        new = update(side, three(0, (0, 1, 2)), wmv, join([first, *first_near]), new)
        new = update(side, last(1, (1, 2), 0) + last(0, (0, 1, 2), 2), wmv, [*later_far, *first_far], new)
        return tuple(a.reshape(b.shape) for a, b in zip(new, arrays, strict=True))

    return jax.shard_map(
        step,
        mesh=mesh,
        in_specs=(P(("rep", "dp"), None, None),) * 2 + (P(None, None, None),) * 9,
        out_specs=(P("rep", None, None),) * 9,
        check_vma=False,
    )
```

```python
import functools
import math

import jax
import jax.numpy as jnp
from jax import lax
from jax.experimental import pallas as pl
from jax.experimental.pallas import tpu as pltpu
from jax.sharding import PartitionSpec as P

MESH = pl.DeviceIdType.MESH
F32, BF16 = jnp.float32, jnp.bfloat16
PANELS = 4
LAT = 2
STAGES = 8
G_SLOTS = 2 * LAT + 2
OUT_SLOTS = 4 * LAT + 3
VMEM_LIMIT = 62 * 2**20


def dot(a, b):
    return jnp.dot(a, b, preferred_element_type=F32)


def dot_t(a, b):
    return lax.dot_general(a, b, (((1,), (1,)), ((), ())), preferred_element_type=F32)


def scale_of(wide):
    return lax.rsqrt(jnp.mean(wide**2, -1, keepdims=True) + 1e-6)


def normed(h):
    wide = h.astype(F32)
    return (wide * scale_of(wide)).astype(BF16)


def at_rows(start, size):
    return pl.ds(pl.multiple_of(start, size), size)


def layers_kernel(side, x_ref, dy_ref, wg_ref, wu_ref, wd_ref, g_ref, *refs):
    later_q, first_q, kept_ref, refs = refs[0:2], refs[2:4], refs[4], refs[5:]
    a_v, at_v, ct_v, acc, wgu, wdb, hidt, dgu, own, part1, done, sbuf, rbuf, x_v, gu_v, sem, wsem, osem, ssem, rsem, ksem = refs
    tokens, d = a_v.shape
    panel = wdb.shape[1]
    blocks = wg_ref.shape[2] // panel
    quarter, unit = panel // side, panel // side // side
    tile = min(512, tokens // 4)
    first, chunks = blocks * 3, 2 * blocks * 3
    half = 3 * quarter + 3 * unit
    X1, X2, Y1, Y2 = 0, quarter, 3 * quarter, 3 * quarter + unit
    AY1, AY2, AX1, AX2 = half, half + 2 * unit, half + 3 * unit, half + 3 * unit + 2 * quarter

    rep, me = lax.axis_index("rep"), lax.axis_index("dp")
    px, py = me // side, me % side
    device = lambda x, y: (rep, (x % side) * side + y % side)
    near = (device(px + 1, py), device(px + side - 1, py), device(px, py + 1), device(px, py + side - 1))
    colours = ((0, (0, 1), (2, 3), px, py), (1, (2, 3), (0, 1), py, px))

    barrier = pltpu.get_barrier_semaphore()
    for n in near:
        pl.semaphore_signal(barrier, inc=1, device_id=n, device_id_type=MESH)

    parts = ((X1, Y1), (Y1, AX1), (AX1, AX2), (AX2, 2 * half))
    sent_in = ((0, chunks + LAT), (2 * LAT, chunks + 5 * LAT), (6 * LAT, first + 6 * LAT), (7 * LAT, first + 7 * LAT))

    def parts_of(k):
        return [which for which in range(4) if which < 2 or (k - (which + 4) * LAT) % 3 == 0]


    def message(link, which, i):
        rows = pl.ds(parts[which][0], parts[which][1] - parts[which][0])
        return pltpu.make_async_remote_copy(
            src_ref=sbuf.at[link, i % LAT, rows],
            dst_ref=rbuf.at[link, i % (2 * LAT), rows],
            send_sem=ssem.at[which, link, i % LAT],
            recv_sem=rsem.at[which, link, i % (2 * LAT)],
            device_id=near[link],
            device_id_type=MESH,
        )

    def take_whole(c):
        pltpu.make_async_copy(done.at[c % OUT_SLOTS], g_ref.at[c // 3], osem.at[c % OUT_SLOTS]).start()

    def take_quarters(k, c, refs):
        slot = c % OUT_SLOTS
        for colour, _, _, p, _ in colours:
            for j in range(2):
                rows = at_rows((2 * colour + j) * panel + p * quarter, quarter)
                to = refs[colour].at[j, k, (c // 3) % blocks]
                pltpu.make_async_copy(done.at[slot, rows], to, osem.at[slot]).start()

    def wait_whole(c):
        pltpu.make_async_copy(done.at[c % OUT_SLOTS], g_ref.at[0], osem.at[c % OUT_SLOTS]).wait()

    def wait_quarters(c):
        rows = pl.ds(0, quarter)
        for _ in range(PANELS):
            pltpu.make_async_copy(done.at[c % OUT_SLOTS, rows], first_q[0].at[0, 0, 0], osem.at[c % OUT_SLOTS]).wait()

    def tick(i, k):
        sent, got = i % LAT, (i + LAT) % (2 * LAT)

        for which in parts_of((k - LAT) % 3):
            start, stop = sent_in[which]

            @pl.when((i >= start + LAT) & (i < stop + LAT))
            def _(which=which):
                for link in range(4):
                    message(link, which, i + LAT).wait_send()
                    message(link, which, i + LAT).wait_recv()

        def stage(s, stop=chunks):
            c = i - s * LAT
            return c, pl.when((c >= 0) & (c < stop))

        def quarter_rows(p, k):
            return at_rows(p * panel + (k % side) * quarter, quarter)

        def unit_rows(p, k, j):
            return at_rows(p * panel + (k % side) * quarter + (j % side) * unit, unit)

        def unit_of(p, j):
            return at_rows(p * quarter + (j % side) * unit, unit)

        wide = lambda v: v.astype(F32)

        c0, when = stage(0)

        @when
        def _():
            for colour, one, two, p, q in colours:
                for j in range(2):
                    sbuf[one[j], sent, pl.ds(X1, quarter)] = own[c0 % G_SLOTS, quarter_rows(2 * colour + j, p + 2)]

        c1, when = stage(1)

        @when
        def _():
            slot = c1 % G_SLOTS
            for colour, one, two, p, q in colours:
                for j in range(2):
                    to = p + (1, side - 1)[j]
                    for w in range(2):
                        v = own[slot, quarter_rows(2 * colour + w, to)]
                        if w == j:
                            v = (wide(v) + wide(rbuf[one[j], got, pl.ds(X1, quarter)])).astype(BF16)
                        sbuf[one[j], sent, pl.ds(X2 + w * quarter, quarter)] = v

        c2, when = stage(2)

        @when
        def _():
            slot = c2 % G_SLOTS
            for colour, one, two, p, q in colours:
                for w in range(2):
                    rows = pl.ds(X2 + w * quarter, quarter)
                    part1[slot, colour, pl.ds(w * quarter, quarter)] = (
                        wide(own[slot, quarter_rows(2 * colour + w, p)]) + wide(rbuf[one[0], got, rows]) + wide(rbuf[one[1], got, rows])
                    )
                for j in range(2):
                    sbuf[two[j], sent, pl.ds(Y1, unit)] = part1[slot, colour, unit_of(j, q + 2)].astype(BF16)

        c3, when = stage(3)

        @when
        def _():
            slot = c3 % G_SLOTS
            for colour, one, two, p, q in colours:
                for j in range(2):
                    to = q + (1, side - 1)[j]
                    for w in range(2):
                        v = part1[slot, colour, unit_of(w, to)]
                        if w == j:
                            v = v + wide(rbuf[two[j], got, pl.ds(Y1, unit)])
                        sbuf[two[j], sent, pl.ds(Y2 + w * unit, unit)] = v.astype(BF16)

        c4, when = stage(4)

        @when
        def _():
            if (k - 4 * LAT - OUT_SLOTS) % 3 == 0:

                @pl.when((c4 >= OUT_SLOTS) & (c4 < first + OUT_SLOTS))
                def _():
                    wait_whole(c4)

                pl.when(c4 >= first + OUT_SLOTS)(lambda: wait_quarters(c4))
            else:
                pl.when(c4 >= OUT_SLOTS)(lambda: wait_quarters(c4))

            slot, to = c4 % G_SLOTS, c4 % OUT_SLOTS
            for colour, one, two, p, q in colours:
                for w in range(2):
                    rows = pl.ds(Y2 + w * unit, unit)
                    v = part1[slot, colour, unit_of(w, q)] + wide(rbuf[two[0], got, rows]) + wide(rbuf[two[1], got, rows])
                    v = v.astype(BF16)
                    done[to, unit_rows(2 * colour + w, p, q)] = v
                    for j in range(2):
                        sbuf[two[j], sent, pl.ds(AY1 + w * unit, unit)] = v

        c5, when = stage(5)

        @when
        def _():
            to = c5 % OUT_SLOTS
            for colour, one, two, p, q in colours:
                for j in range(2):
                    for w in range(2):
                        v = rbuf[two[j], got, pl.ds(AY1 + w * unit, unit)]
                        done[to, unit_rows(2 * colour + w, p, q + (side - 1, 1)[j])] = v
                        if w == j:
                            sbuf[two[j], sent, pl.ds(AY2, unit)] = v

        c6, when = stage(6)

        @when
        def _():
            to = c6 % OUT_SLOTS
            for colour, one, two, p, q in colours:
                for j in range(2):
                    done[to, unit_rows(2 * colour + j, p, q + 2)] = rbuf[two[j], got, pl.ds(AY2, unit)]

            kind = (k - 6 * LAT) % 3

            @pl.when(c6 < first)
            def _():
                if kind:
                    take_quarters(kind - 1, c6, later_q)
                else:
                    for colour, one, two, p, q in colours:
                        for w in range(2):
                            v = done[to, quarter_rows(2 * colour + w, p)]
                            for j in range(2):
                                sbuf[one[j], sent, pl.ds(AX1 + w * quarter, quarter)] = v

            pl.when(c6 >= first)(lambda: take_quarters(kind, c6, first_q))

        c7, when = stage(7, first)

        def spread():
            to = c7 % OUT_SLOTS
            for colour, one, two, p, q in colours:
                for j in range(2):
                    for w in range(2):
                        v = rbuf[one[j], got, pl.ds(AX1 + w * quarter, quarter)]
                        done[to, quarter_rows(2 * colour + w, p + (side - 1, 1)[j])] = v
                        if w == j:
                            sbuf[one[j], sent, pl.ds(AX2, quarter)] = v

        if (k - 7 * LAT) % 3 == 0:
            when(spread)

        c8, when = stage(8, first)

        def finish():
            to = c8 % OUT_SLOTS
            for colour, one, two, p, q in colours:
                for j in range(2):
                    done[to, quarter_rows(2 * colour + j, p + 2)] = rbuf[one[j], got, pl.ds(AX2, quarter)]
            take_whole(c8)

        if (k - 8 * LAT) % 3 == 0:
            when(finish)

        for which in parts_of(k):
            start, stop = sent_in[which]

            @pl.when((i >= start) & (i < stop))
            def _(which=which):
                for link in range(4):
                    message(link, which, i).start()

    def weights(turn):
        slot, layer, cols = turn % 2, (turn // blocks) % 2, at_rows((turn % blocks) * panel, panel)
        return (
            pltpu.make_async_copy(wg_ref.at[layer, :, cols], wgu.at[slot, :, pl.ds(0, panel)], wsem.at[0, slot]),
            pltpu.make_async_copy(wu_ref.at[layer, :, cols], wgu.at[slot, :, pl.ds(panel, panel)], wsem.at[1, slot]),
            pltpu.make_async_copy(wd_ref.at[layer, cols, :], wdb.at[slot], wsem.at[2, slot]),
        )

    def take_in(_t, _):
        rows = at_rows(_t * tile, tile)
        a = normed(a_v[rows, :])
        a_v[rows, :] = a
        at_v[:, rows] = a.T
        return _

    def columns_of(number):
        return at_rows((number % 2) * 2 * panel, 2 * panel)

    def fetch(number):
        return pltpu.make_async_copy(kept_ref.at[number - blocks], acc.at[:, columns_of(number)], sem.at[number % 2])

    def keep(b):
        return pltpu.make_async_copy(gu_v.at[b % 2], kept_ref.at[b], ksem.at[b % 2])

    gets = (pltpu.make_async_copy(x_ref, x_v, sem.at[0]), pltpu.make_async_copy(dy_ref, ct_v, sem.at[1]))
    gets[0].start()
    for c in weights(0):
        c.start()
    gets[0].wait()
    gets[1].start()

    def first_norm(t, _):
        rows = at_rows(t * tile, tile)
        a_v[rows, :] = normed(x_v[rows, :])
        acc[rows, :] = jnp.zeros((tile, d), F32)
        return _

    lax.fori_loop(0, tokens // tile, first_norm, 0)

    def forward(b, carry):
        slot = b % 2
        for c in weights(b):
            c.wait()
        for c in weights(b + 1):
            c.start()

        @pl.when(b >= 2)
        def _():
            keep(b).wait()

        for t in range(tokens // tile):
            rows = pl.ds(t * tile, tile)
            gu = dot(a_v[rows, :], wgu[slot])
            gu_v[slot, rows, :] = gu
            hidden = (jax.nn.silu(gu[:, :panel]) * gu[:, panel:]).astype(BF16)
            acc[rows, :] += dot(hidden, wdb[slot])
        keep(b).start()
        return carry

    lax.fori_loop(0, blocks, forward, 0)

    def between(t, _):
        rows = at_rows(t * tile, tile)
        x_v[rows, :] = x_v[rows, :] + acc[rows, :].astype(BF16)
        a = normed(x_v[rows, :])
        a_v[rows, :] = a
        at_v[:, rows] = a.T
        return _

    lax.fori_loop(0, tokens // tile, between, 0)
    for b in range(max(0, blocks - 2), blocks):
        keep(b).wait()
    gets[1].wait()
    pl.semaphore_wait(barrier, 4)

    def next_layer():
        get = pltpu.make_async_copy(x_ref, a_v, sem.at[0])
        get.start()
        small = tile // 4

        def back(t, _):
            rows = at_rows(t * small, small)
            wide = x_v[rows, :].astype(F32)
            scale = scale_of(wide)
            by_a = acc[rows, :].astype(BF16).astype(F32)
            inner = jnp.mean(by_a * wide, -1, keepdims=True)
            by_h = by_a * scale - wide * (scale * scale * scale * inner)
            ct_v[rows, :] = ct_v[rows, :] + by_h.astype(BF16)
            return _

        lax.fori_loop(0, tokens // small, back, 0)
        get.wait()
        fetch(blocks).start()
        lax.fori_loop(0, tokens // tile, take_in, 0)

    def block(number, carry):
        turn = blocks + number
        slot = turn % 2
        later = number < blocks
        i = 3 * number

        pl.when(number == blocks)(next_layer)

        for c in weights(turn):
            c.wait()

        @pl.when(number + 1 < 2 * blocks)
        def _():
            for c in weights(turn + 1):
                c.start()

        @pl.when(number >= blocks)
        def _():
            pltpu.make_async_copy(kept_ref.at[0], acc.at[:, columns_of(number)], sem.at[number % 2]).wait()

            @pl.when(number + 1 < 2 * blocks)
            def _():
                fetch(number + 1).start()

        def hidden(t, gu):
            rows = pl.ds(t * tile, tile)
            by_hidden = dot_t(ct_v[rows, :], wdb[slot]).astype(BF16).astype(F32)
            gate, up = gu[:, :panel], gu[:, panel:]
            sigmoid = jax.nn.sigmoid(gate)
            silu = gate * sigmoid
            hidt[:, rows] = (silu * up).astype(BF16).T
            dgu[rows, pl.ds(0, panel)] = (by_hidden * up * (sigmoid + silu * (1.0 - sigmoid))).astype(BF16)
            dgu[rows, pl.ds(panel, panel)] = (by_hidden * silu).astype(BF16)

        def hidden_half(part):
            tiles = tokens // tile // 2

            @pl.when(later)
            def _():
                for t in range(part * tiles, part * tiles + tiles):
                    hidden(t, dot(a_v[pl.ds(t * tile, tile), :], wgu[slot]))

            @pl.when(number >= blocks)
            def _():
                for t in range(part * tiles, part * tiles + tiles):
                    hidden(t, acc[pl.ds(t * tile, tile), columns_of(number)])

        hidden_half(0)

        @pl.when(number > 0)
        def _():
            tick(i - 1, 2)

        hidden_half(1)
        for k in range(PANELS):
            own[i % G_SLOTS, pl.ds(k * panel, panel)] = dot(hidt[...], ct_v[:, pl.ds(k * panel, panel)]).astype(BF16)
        tick(i, 0)
        for k in range(PANELS):
            v = dot(at_v[pl.ds(k * panel, panel), :], dgu[...]).astype(BF16)
            own[(i + 1) % G_SLOTS, pl.ds(k * panel, panel)] = v[:, :panel]
            own[(i + 2) % G_SLOTS, pl.ds(k * panel, panel)] = v[:, panel:]
        tick(i + 1, 1)

        @pl.when(later)
        def _():
            for t in range(tokens // tile):
                rows = pl.ds(t * tile, tile)
                v = dot_t(dgu[rows, :], wgu[slot])
                acc[rows, :] = jnp.where(number == 0, v, acc[rows, :] + v)

        return carry

    lax.fori_loop(0, 2 * blocks, block, 0)

    tick(chunks - 1, 2)

    def drain(t, _):
        for k in range(3):
            tick(chunks + 3 * t + k, k)
        return _

    lax.fori_loop(0, (6 * LAT + 2) // 3, drain, 0)
    for c in range(chunks - OUT_SLOTS, chunks):
        (wait_whole if c < first and c % 3 == 0 else wait_quarters)(c)


def run_layers(side, x, dy, wg, wu, wd):
    tokens, d = x.shape
    panel = d // PANELS
    blocks = wg.shape[2] // panel
    rows = 6 * (panel // side + panel // side // side)
    hbm = pl.BlockSpec(memory_space=pl.ANY)
    return pl.pallas_call(
        functools.partial(layers_kernel, side),
        out_shape=(jax.ShapeDtypeStruct((blocks, d, panel), BF16),)
        + tuple(jax.ShapeDtypeStruct((2, n, blocks, panel // side, panel), BF16) for n in (2, 3) for _ in range(2))
        + (jax.ShapeDtypeStruct((blocks, tokens, 2 * panel), F32),),
        in_specs=[hbm] * 5,
        out_specs=(hbm,) * 6,
        scratch_shapes=[
            pltpu.VMEM((tokens, d), BF16),
            pltpu.VMEM((d, tokens), BF16),
            pltpu.VMEM((tokens, d), BF16),
            pltpu.VMEM((tokens, d), F32),
            pltpu.VMEM((2, d, 2 * panel), BF16),
            pltpu.VMEM((2, panel, d), BF16),
            pltpu.VMEM((panel, tokens), BF16),
            pltpu.VMEM((tokens, 2 * panel), BF16),
            pltpu.VMEM((G_SLOTS, d, panel), BF16),
            pltpu.VMEM((G_SLOTS, 2, 2 * panel // side, panel), F32),
            pltpu.VMEM((OUT_SLOTS, d, panel), BF16),
            pltpu.VMEM((4, LAT, rows, panel), BF16),
            pltpu.VMEM((4, 2 * LAT, rows, panel), BF16),
            pltpu.VMEM((tokens, d), BF16),
            pltpu.VMEM((2, tokens, 2 * panel), F32),
            pltpu.SemaphoreType.DMA((2,)),
            pltpu.SemaphoreType.DMA((3, 2)),
            pltpu.SemaphoreType.DMA((OUT_SLOTS,)),
            pltpu.SemaphoreType.DMA((4, 4, LAT)),
            pltpu.SemaphoreType.DMA((4, 4, 2 * LAT)),
            pltpu.SemaphoreType.DMA((2,)),
        ],
        compiler_params=pltpu.CompilerParams(collective_id=0, has_side_effects=True, vmem_limit_bytes=VMEM_LIMIT),
        cost_estimate=pl.CostEstimate(flops=30 * tokens * d * wg.shape[2], bytes_accessed=4 * 3 * wg.size, transcendentals=2 * tokens * wg.shape[2]),
        name="layers",
    )(x, dy, wg, wu, wd)


def adamw(w, m, v, g):
    m = 0.9 * m + 0.1 * g
    v = 0.95 * v + 0.05 * g * g
    step = m * lax.rsqrt(v + 1e-8) + 0.1 * w
    return (w - 0.02 * step).astype(BF16), m, v


RING = 4
AHEAD = 2


def update_kernel(side, plan, sources, fresh, *refs):
    wmv, refs = (refs[0:3], refs[3:6], refs[6:9]), refs[9:]
    source, refs = refs[:sources], refs[sources:]
    refs = refs if fresh else refs[9:]
    new, refs = (refs[0:3], refs[3:6], refs[6:9]), refs[9:]
    tall, flat, gbuf, isem, osem = refs[0:3], refs[3:6], refs[6], refs[7], refs[8]
    _, quarter, panel = gbuf.shape[2:]
    me = lax.axis_index("dp")
    position = (me // side, me % side)
    units = plan

    def arrays(refs, u):
        layer, kind, start, blocks, colour, k, relative, _ = units[u]
        k = (position[colour] + k + side) % side if relative else k
        if kind == 0:
            at = (layer, pl.ds(start, blocks), k, slice(None), pl.ds(2 * colour * panel, 2 * panel))
        else:
            at = (layer, pl.ds(2 * colour, 2), k, slice(None), pl.ds(start * panel, blocks * panel))
        return [r[(2, 0, 1)[kind]].at[at] for r in refs]

    def buffers(u):
        blocks = units[u][3]
        if units[u][1] == 0:
            return [b.at[u % RING, pl.ds(0, blocks)] for b in flat]
        return [b.at[u % RING, :, :, pl.ds(0, blocks * panel)] for b in tall]

    def copies_in(u):
        _, _, start, blocks, _, _, _, halves = units[u]
        slot = u % RING
        cs = [pltpu.make_async_copy(a, b, isem.at[n, slot]) for n, (a, b) in enumerate(zip(arrays(wmv, u), buffers(u)))]
        for j, (which, index, rows) in enumerate(halves):
            ref = source[which] if index is None else source[which].at[index]
            ref = ref.at[pl.ds(start, blocks), pl.ds(rows, quarter)]
            cs.append(pltpu.make_async_copy(ref, gbuf.at[slot, j, pl.ds(0, blocks)], isem.at[3 + j, slot]))
        return cs

    def copies_out(u):
        return [pltpu.make_async_copy(b, a, osem.at[n, u % RING]) for n, (a, b) in enumerate(zip(arrays(new, u), buffers(u)))]

    def begin(u):
        for c in copies_in(u):
            c.start()

    for u in range(min(AHEAD, len(units))):
        begin(u)
    for u in range(len(units)):
        if u + AHEAD < len(units):
            if u + AHEAD >= RING:
                for c in copies_out(u + AHEAD - RING):
                    c.wait()
            begin(u + AHEAD)
        for c in copies_in(u):
            c.wait()
        slot = u % RING
        w_b, m_b, v_b = flat if units[u][1] == 0 else tall

        def part(b, carry):
            for j in range(2):
                if units[u][1] == 0:
                    at = (slot, b, slice(None), pl.ds(j * panel, panel))
                else:
                    at = (slot, j, slice(None), at_rows(b * panel, panel))
                w_b[at], m_b[at], v_b[at] = adamw(w_b[at].astype(F32), m_b[at], v_b[at], gbuf[slot, j, b].astype(F32))
            return carry

        lax.fori_loop(0, units[u][3], part, 0)
        for c in copies_out(u):
            c.start()
    for u in range(max(0, len(units) - RING), len(units)):
        for c in copies_out(u):
            c.wait()


def update(side, plan, wmv, sources, old):
    _, _, _, quarter, ff = wmv[0].shape
    blocks = max(one[3] for one in plan)
    panel = ff // wmv[2].shape[1]
    hbm = pl.BlockSpec(memory_space=pl.ANY)
    size = sum(one[3] for one in plan) * 2 * quarter * panel
    return pl.pallas_call(
        functools.partial(update_kernel, side, plan, len(sources), old is None),
        out_shape=tuple(jax.ShapeDtypeStruct(a.shape, a.dtype) for a in wmv),
        in_specs=[hbm] * (9 + len(sources) + (0 if old is None else 9)),
        out_specs=(hbm,) * 9,
        input_output_aliases={} if old is None else {9 + len(sources) + n: n for n in range(9)},
        scratch_shapes=[pltpu.VMEM((RING, 2, quarter, blocks * panel), t) for t in (BF16, F32, F32)]
        + [pltpu.VMEM((RING, blocks, quarter, 2 * panel), t) for t in (BF16, F32, F32)]
        + [pltpu.VMEM((RING, 2, blocks, quarter, panel), BF16), pltpu.SemaphoreType.DMA((5, RING)), pltpu.SemaphoreType.DMA((3, RING))],
        compiler_params=pltpu.CompilerParams(vmem_limit_bytes=VMEM_LIMIT),
        cost_estimate=pl.CostEstimate(flops=size * 6000, bytes_accessed=22 * size, transcendentals=size),
        name="update",
    )(*wmv, *sources, *(old or ()))


def solution(mesh):
    side = math.isqrt(mesh.shape["dp"])
    spots = [(x, y) for x in range(side) for y in range(side)]

    def shift(dx, dy):
        return [(x * side + y, (x + dx) % side * side + (y + dy) % side) for x, y in spots]

    ways = ((shift(1, 0), shift(-1, 0)), (shift(0, 1), shift(0, -1)))

    def step(x, dy, *arrays):
        weights = arrays[:3]
        x, dy = x[0], dy[0]
        d, ff = weights[0].shape[1:]
        panel = d // PANELS
        quarter, blocks = panel // side, ff // panel
        whole, *quarters, _ = run_layers(side, x, dy, *weights)
        wmv = [a.reshape(a.shape[0], blocks, side, quarter, d) if n % 3 == 2 else a.reshape(a.shape[0], PANELS, side, quarter, ff) for n, a in enumerate(arrays)]

        def near(quarters):
            return [[lax.ppermute(q, "dp", ways[c][way]) for c, q in enumerate(quarters)] for way in range(2)]

        def far(near, way):
            return [lax.ppermute(q, "dp", ways[c][way]) for c, q in enumerate(near[way])]

        def pieces(layer, kinds, colour, k, relative, halves):
            return [(layer, kind, 0, blocks, colour, k, relative, halves(kind)) for kind in kinds]

        def join(parts):
            return [one for part in parts for one in part]

        def three(layer, kinds):
            return join(
                pieces(layer, kinds, c, r, True, lambda kind: [(2 * s + c, (j, kind - kinds[0]), 0) for j in range(2)])
                for c in range(2)
                for s, r in enumerate((0, -1, 1))
            )

        def last(layer, kinds, at):
            return join(pieces(layer, kinds, c, 2, True, lambda kind: [(at + c, (j, kind - kinds[0]), 0) for j in range(2)]) for c in range(2))

        def known(layer, kind):
            return join(
                pieces(layer, (kind,), c, k, False, lambda _: [(0, None, (2 * c + j) * panel + k * quarter) for j in range(2)])
                for c in range(2)
                for k in range(side)
            )

        later, first = quarters[:2], quarters[2:]
        later_near, first_near = near(later), near(first)
        new = update(side, known(1, 0), wmv, [whole], None)
        later_far = far(later_near, 0)
        early = pieces(0, (0, 1, 2), 0, 0, True, lambda kind: [(6, (j, kind), 0) for j in range(2)])
        new = update(side, three(1, (1, 2)) + early, wmv, join([later, *later_near]) + first[:1], new)
        first_far = far(first_near, 1)
        remaining = [one for one in three(0, (0, 1, 2)) if one[4:6] != (0, 0)]
        new = update(side, remaining, wmv, join([first, *first_near]), new)
        new = update(side, last(1, (1, 2), 0), wmv, later_far, new)
        new = update(side, last(0, (0, 1, 2), 0), wmv, first_far, new)
        return tuple(a.reshape(b.shape) for a, b in zip(new, arrays, strict=True))

    return jax.shard_map(
        step,
        mesh=mesh,
        in_specs=(P(("rep", "dp"), None, None),) * 2 + (P(None, None, None),) * 9,
        out_specs=(P("rep", None, None),) * 9,
        check_vma=False,
    )
```
